256 devices in a mesh: dp: 256 (over y, x, z, core).
Axes of the slice: x: 4, y: 4, z: 8, core: 2. Of those that a mesh axis runs over, the one named last changes fastest.
Arguments:
- features: bfloat16 [2048, 128, 1024], P('dp'), may hold values from -16 to 16
- ln_gain: float32 [1024], replicated, may hold values from 0.5 to 1.5
- w_query: bfloat16 [1024, 1024], replicated, may hold values from -0.1875 to 0.1875
- w_key: bfloat16 [1024, 1024], replicated, may hold values from -0.1875 to 0.1875
- w_value: bfloat16 [1024, 1024], replicated, may hold values from -0.1875 to 0.1875
- w_out: bfloat16 [1024, 1024], replicated, may hold values from -0.1875 to 0.1875
- text_raw: bfloat16 [2048, 1024], P('dp'), may hold values from -0.35 to 0.35
Outputs:
- loss: float32 [], replicated
- text_grad: float32 [2048, 1024], P('dp')
- w_out_grad: bfloat16 [1024, 1024], replicated
The draws below stay inside these ranges and needn't reach their ends.
All inputs are finite; a program needn't handle non-finite values.
Results may differ from the reference program's by a relative error of at most 0.009.
Values may be sent and summed in bfloat16 or wider, within the bound.
A program may use at most 128 MiB of HBM per device.

```python
import jax
import jax.numpy as jnp
from jax import lax

D = 1024
HEADS = 16
PATCHES = 127
BATCH = 2048


def unit_noise(rng_key, shape):
    return jax.random.truncated_normal(rng_key, -4.0, 4.0, shape, jnp.float32)


def paired_rows(key):
    folded = jax.random.fold_in(key, 1031)
    streams = jax.random.split(folded, 7)
    common = unit_noise(streams[0], (1, D))
    shared = unit_noise(streams[1], (BATCH, D))
    image_noise = unit_noise(streams[2], (BATCH, D))
    text_noise = unit_noise(streams[3], (BATCH, D))
    order = jax.random.permutation(streams[6], BATCH).astype(jnp.int32)
    partner = jnp.zeros((BATCH,), jnp.int32).at[order].set(jnp.roll(order, -1))
    mate_rows = shared[partner]
    ramp = jnp.arange(BATCH, dtype=jnp.float32)[:, None] / BATCH
    image_scale = jax.random.uniform(streams[4], (BATCH, 1), jnp.float32, 0.3, 0.7)
    text_scale = jax.random.uniform(streams[5], (BATCH, 1), jnp.float32, 0.0, 0.9)
    noise_scale = 0.4 + 1.6 * ramp
    class_rows = image_scale * common + shared + 0.7 * mate_rows + noise_scale * image_noise
    text_rows = 0.03125 * (text_scale * common + shared + 0.8 * text_noise)
    return (class_rows, text_rows)


def draw_features(key, part):
    class_rows, text_rows = paired_rows(key)
    patch_rows = unit_noise(jax.random.fold_in(key, 2063), (BATCH, PATCHES, D))
    return jnp.concatenate([class_rows[:, None, :], patch_rows], axis=1).astype(jnp.bfloat16)


def draw_text_raw(key, part):
    class_rows, text_rows = paired_rows(key)
    return text_rows.astype(jnp.bfloat16)


def normal_values(key, extent, scale, bound, kind=jnp.bfloat16):
    entries = scale * jax.random.normal(key, extent, jnp.float32)
    return jnp.clip(entries, min=-bound, max=bound).astype(kind)


def setup_inputs(seed: int = 0) -> dict:
    key_of = jax.random.split(jax.random.key(seed), 8)
    return {
        "features": draw_features(jax.random.fold_in(key_of[7], 71), 0),
        "ln_gain": jnp.clip(1.0 + 0.1 * jax.random.normal(key_of[1], (D,), jnp.float32), 0.5, 1.5),
        "w_query": normal_values(key_of[2], (D, D), D ** -0.5, 0.1875),
        "w_key": normal_values(key_of[3], (D, D), D ** -0.5, 0.1875),
        "w_value": normal_values(key_of[4], (D, D), D ** -0.5, 0.1875),
        "w_out": normal_values(key_of[5], (D, D), D ** -0.5, 0.1875),
        "text_raw": draw_text_raw(jax.random.fold_in(key_of[7], 71), 0),
    }


inv_temp = 1.0 / 0.07
attn_temp = 8.0
epsilon = 1e-06

def layer_norm(inputs, gain):
    center = inputs - lax.optimization_barrier(jnp.mean(inputs, axis=-1, keepdims=True))
    spread = lax.optimization_barrier(jnp.mean(center * center, axis=-1, keepdims=True))
    return center * lax.rsqrt(spread + epsilon) * gain

def unit_heads(proj, heads):
    shaped = proj.reshape(proj.shape[0], proj.shape[1], heads, -1)
    return (shaped * lax.rsqrt(lax.optimization_barrier(jnp.sum(shaped * shaped, axis=-1, keepdims=True)) + epsilon)).astype(jnp.bfloat16)

def embed(feats, ln_gain, w_query, w_key, w_value, w_out):
    images, tokens, width = feats.shape
    inputs = feats.astype(jnp.float32)
    normed = layer_norm(inputs, ln_gain).astype(jnp.bfloat16).reshape(images * tokens, width)
    query = unit_heads(jnp.dot(normed, w_query, preferred_element_type=jnp.float32).reshape(images, tokens, width), HEADS)
    key_heads = unit_heads(jnp.dot(normed, w_key, preferred_element_type=jnp.float32).reshape(images, tokens, width), HEADS)
    value_heads = jnp.dot(normed, w_value, preferred_element_type=jnp.float32).reshape(images, tokens, HEADS, -1).astype(jnp.bfloat16)
    scores = attn_temp * jnp.einsum('bqhd,bkhd->bhqk', query.astype(jnp.float32), key_heads.astype(jnp.float32))
    expo = jnp.exp(scores)
    weights = (expo / lax.optimization_barrier(jnp.sum(expo, axis=-1, keepdims=True))).astype(jnp.bfloat16).astype(jnp.float32)
    pooled = weights[:, :, 0, :] + lax.optimization_barrier(jnp.mean(weights[:, :, 1:, :], axis=2))
    abar = jnp.einsum('bhk,bkhd->bhd', pooled, value_heads.astype(jnp.float32), precision=lax.Precision.HIGHEST)
    abar = abar.reshape(images, width).astype(jnp.bfloat16)
    xbar = inputs[:, 0, :] + lax.optimization_barrier(jnp.mean(inputs[:, 1:, :], axis=1))
    emb = xbar + jnp.dot(abar, w_out, preferred_element_type=jnp.float32)
    return (emb, abar)

def reference(features, ln_gain, w_query, w_key, w_value, w_out, text_raw):

    def one_image(single):
        return embed(single[None], ln_gain, w_query, w_key, w_value, w_out)
    emb, abar = lax.map(one_image, features)
    emb = emb.reshape(BATCH, D)
    abar = abar.reshape(BATCH, D)
    emb_norm = jnp.sqrt(lax.optimization_barrier(jnp.sum(emb * emb, axis=1, keepdims=True)) + epsilon)
    img_f = emb / emb_norm
    img_u = img_f.astype(jnp.bfloat16)
    text32 = text_raw.astype(jnp.float32)
    txt_norm = jnp.sqrt(lax.optimization_barrier(jnp.sum(text32 * text32, axis=1, keepdims=True)) + epsilon)
    txt_f = text32 / txt_norm
    txt_u = txt_f.astype(jnp.bfloat16)
    logits = inv_temp * jnp.dot(img_u, txt_u.T, preferred_element_type=jnp.float32)
    exp_logits = jnp.exp(logits)
    rowsum = lax.optimization_barrier(jnp.sum(exp_logits, axis=1))
    colsum = lax.optimization_barrier(jnp.sum(exp_logits, axis=0))
    diag_logit = jnp.diagonal(logits)
    loss = (jnp.sum(jnp.log(rowsum) - diag_logit) + jnp.sum(jnp.log(colsum) - diag_logit)) / (2.0 * BATCH)
    delta = 0.5 * (exp_logits / rowsum[:, None] + exp_logits / colsum[None, :]) - jnp.eye(BATCH, dtype=jnp.float32)
    delta = delta.astype(jnp.bfloat16)
    grad_img = inv_temp * jnp.dot(delta, txt_u, preferred_element_type=jnp.float32)
    grad_txt = inv_temp * jnp.dot(delta.T, img_u, preferred_element_type=jnp.float32)
    text_grad = (grad_txt - txt_f * lax.optimization_barrier(jnp.sum(txt_f * grad_txt, axis=1, keepdims=True))) / txt_norm
    emb_grad = (grad_img - img_f * lax.optimization_barrier(jnp.sum(img_f * grad_img, axis=1, keepdims=True))) / emb_norm
    w_out_grad = jnp.dot(abar.astype(jnp.float32).T, emb_grad, precision=lax.Precision.HIGHEST).astype(jnp.bfloat16)
    return (loss, text_grad, w_out_grad)
```

```python
import functools

import jax
import jax.numpy as jnp
from jax import lax
from jax.experimental import pallas as pl
from jax.experimental.pallas import tpu as pltpu
from jax.sharding import PartitionSpec as P

INV_TEMP = 1.0 / 0.07
EPS = 1e-06
LOG2E = 1.4426950408889634
F32 = jnp.float32
BF16 = jnp.bfloat16
MESH = pl.DeviceIdType.MESH
NT = (((1,), (1,)), ((), ()))
TN = (((0,), (0,)), ((), ()))
NN = (((1,), (0,)), ((), ()))


def dot(a, b, dims=NN):
    return lax.dot_general(a, b, dims, preferred_element_type=F32)


def iota(shape, dim):
    return lax.broadcasted_iota(jnp.int32, shape, dim)


def embed_kernel(
    feat_hbm, gain_ref, wq_hbm, wk_hbm, wv_hbm, wo_hbm, emb_ref, abar_ref,
    feat, wq, wk, wv, wo, normed, qh, kh, vh, abar, xbar, fsem, wsem,
):
    images = feat.shape[0]
    fcopy = [
        pltpu.make_async_copy(feat_hbm.at[i], feat.at[i], fsem.at[i]) for i in range(images)
    ]
    pairs = ((wq_hbm, wq), (wk_hbm, wk), (wv_hbm, wv), (wo_hbm, wo))
    wcopy = [pltpu.make_async_copy(s, d, wsem.at[i]) for i, (s, d) in enumerate(pairs)]
    for cp in fcopy + wcopy:
        cp.start()
    gain = gain_ref[...]

    for i in range(images):
        fcopy[i].wait()

        def norm_rows(t, total, i=i):
            rows = pl.ds(pl.multiple_of(t * 32, 32), 32)
            x = feat[i, rows, :].astype(F32)
            center = x - jnp.mean(x, axis=-1, keepdims=True)
            spread = jnp.mean(center * center, axis=-1, keepdims=True)
            out = center * lax.rsqrt(spread + EPS) * gain
            normed[pl.ds(pl.multiple_of(i * 128 + t * 32, 32), 32), :] = out.astype(BF16)
            return total + jnp.sum(x.reshape(4, 8, 1024), axis=0)

        total = lax.fori_loop(0, 4, norm_rows, jnp.zeros((8, 1024), F32))
        total = jnp.sum(total, axis=0, keepdims=True)
        first = feat[i, 0:16, :].astype(F32)[0:1]
        xbar[i : i + 1, :] = first + (total - first) * (1.0 / 127.0)

    same_head = jnp.where(
        iota((256, 256), 0) // 64 == iota((256, 256), 1) // 64, 1.0, 0.0
    ).astype(BF16)

    def project(w, out, scale):
        def step(t, carry):
            rows = pl.ds(pl.multiple_of((t % 2) * 512, 512), 512)
            cols = pl.ds(pl.multiple_of((t // 2) * 256, 256), 256)
            proj = dot(normed[rows, :], w[:, cols])
            if scale is not None:
                squares = dot((proj * proj).astype(BF16), same_head)
                proj = proj * (lax.rsqrt(squares + EPS) * scale)
            out[rows, cols] = proj.astype(BF16)
            return carry

        lax.fori_loop(0, 8, step, 0)

    wcopy[0].wait()
    project(wq, qh, 8.0 * LOG2E)
    wcopy[1].wait()
    project(wk, kh, 1.0)
    wcopy[2].wait()
    project(wv, vh, None)

    lane = iota((1, 128), 1)
    low = jnp.where(lane < 64, 1.0, 0.0).astype(BF16)
    high = jnp.where(lane < 64, 0.0, 1.0).astype(BF16)
    share = jnp.where(iota((1, 256), 1) % 128 == 0, 1.0, 1.0 / 127.0).astype(F32)
    gather = jnp.where(
        iota((256, 128), 0) // 128 == iota((256, 128), 1) // 64, 1.0, 0.0
    ).astype(BF16)

    def attend(i, carry):
        rows = pl.ds(pl.multiple_of(i * 128, 128), 128)
        parts = []
        for p in range(8):
            cols = slice(p * 128, p * 128 + 128)
            q = qh[rows, cols]
            both = jnp.concatenate([q * low, q * high], axis=0)
            expo = jnp.exp2(dot(kh[rows, cols], both, NT))
            weight = share / jnp.sum(expo, axis=0, keepdims=True)
            pooled = dot((expo * weight).astype(BF16), gather)
            parts.append(jnp.sum(pooled * vh[rows, cols].astype(F32), axis=0, keepdims=True))
        abar[pl.ds(i, 1), :] = jnp.concatenate(parts, axis=1)
        return carry

    lax.fori_loop(0, images, attend, 0)
    rounded = abar[...].astype(BF16)
    abar_ref[...] = abar[...]
    wcopy[3].wait()
    emb_ref[...] = xbar[...] + dot(rounded, wo[...])


def embed(features, gain, wq, wk, wv, wo):
    images, tokens, width = features.shape
    rows = images * tokens
    any_spec = pl.BlockSpec(memory_space=pl.ANY)
    vmem = pl.BlockSpec(memory_space=pltpu.VMEM)
    square = pltpu.VMEM((width, width), BF16)
    return pl.pallas_call(
        embed_kernel,
        out_shape=[
            jax.ShapeDtypeStruct((images, width), F32),
            jax.ShapeDtypeStruct((images, width), F32),
        ],
        in_specs=[any_spec, vmem, any_spec, any_spec, any_spec, any_spec],
        out_specs=[vmem, vmem],
        scratch_shapes=[
            pltpu.VMEM((images, tokens, width), BF16),
            square, square, square, square,
            pltpu.VMEM((rows, width), BF16),
            pltpu.VMEM((rows, width), BF16),
            pltpu.VMEM((rows, width), BF16),
            pltpu.VMEM((rows, width), BF16),
            pltpu.VMEM((images, width), F32),
            pltpu.VMEM((images, width), F32),
            pltpu.SemaphoreType.DMA((images,)),
            pltpu.SemaphoreType.DMA((4,)),
        ],
        compiler_params=pltpu.CompilerParams(vmem_limit_bytes=48 << 20),
        name="embed",
    )(features, gain, wq, wk, wv, wo)


def pack_rows(col):
    lane = iota((8, 128), 1)
    tile = jnp.zeros((8, 128), F32)
    for k in range(8):
        tile = jnp.where(lane == k, col[8 * k : 8 * k + 8], tile)
    return tile


def unpack_rows(tile):
    return jnp.concatenate([tile[:, k : k + 1] for k in range(8)], axis=0)


def loss_kernel(
    emb_ref, abar_ref, text_ref, wgrad, tgrad_ref, loss_ref,
    t_all, u_all, a_all, rs_all, cs_all, g_send, g_recv, s_all,
    h_send, h_recv, w_send, w_recv, l_all, send, recv, c1, c2,
):
    idx = lax.axis_index("dp")
    core = idx % 2
    z = (idx // 2) % 8
    x = (idx // 16) % 4
    y = idx // 64
    c = x * 2 + core
    r = y * 8 + z

    def row_peer(k):
        p = (c + k) % 8
        return p, (y * 64 + (p // 2) * 16 + z * 2 + p % 2,)

    def col_peer(k):
        p = (r + k) % 32
        return p, ((p // 8) * 64 + x * 16 + (p % 8) * 2 + core,)

    a = y * (1 - core) + x * core
    b = x * (1 - core) + y * core

    def place(a1, b1):
        y1 = a1 * (1 - core) + b1 * core
        x1 = b1 * (1 - core) + a1 * core
        return y1, x1

    def device(a1, b1, z1, core1):
        y1, x1 = place(a1, b1)
        return (y1 * 64 + x1 * 16 + z1 * 2 + core1,)

    def plane_peer(k):
        p = (a * 8 + z + k) % 32
        return p, device(p // 8, b, p % 8, core)

    barrier = pltpu.get_barrier_semaphore()

    def greet(peer):
        def step(k, carry):
            pl.semaphore_signal(barrier, inc=1, device_id=peer(k)[1], device_id_type=MESH)
            return carry

        return step

    lax.fori_loop(1, 8, greet(row_peer), 0)
    lax.fori_loop(1, 32, greet(col_peer), 0)
    lax.fori_loop(1, 32, greet(plane_peer), 0)

    def push(src, dst, s, dev):
        pltpu.make_async_remote_copy(
            src_ref=src, dst_ref=dst, send_sem=send.at[s], recv_sem=recv.at[s],
            device_id=dev, device_id_type=MESH,
        ).start()

    def share(buf, slot, s, peer, n):
        def step(k, carry):
            push(buf.at[slot], buf.at[slot], s, peer(k)[1])
            return carry

        lax.fori_loop(1, n, step, 0)

    def scatter(src, dst, slot, s, peer, n):
        def step(k, carry):
            p, dev = peer(k)
            push(src.at[p], dst.at[slot], s, dev)
            return carry

        lax.fori_loop(1, n, step, 0)

    def local(src, dst, sem):
        return pltpu.make_async_copy(src, dst, sem)

    def arrived(buf, s, n):
        part = buf.at[pl.ds(0, n - 1)]
        local(part, part, recv.at[s]).wait()

    def left(buf, s, n):
        part = buf.at[pl.ds(0, n - 1)]
        local(part, part, send.at[s]).wait()

    text = text_ref[...].astype(F32)
    txt_norm = jnp.sqrt(jnp.sum(text * text, axis=1, keepdims=True) + EPS)
    txt_f = text / txt_norm
    txt_u = txt_f.astype(BF16)
    t_all[r] = txt_u
    emb = emb_ref[...]
    emb_norm = jnp.sqrt(jnp.sum(emb * emb, axis=1, keepdims=True) + EPS)
    img_u = (emb / emb_norm).astype(BF16)
    u_all[c] = img_u
    abar = abar_ref[...].astype(BF16).astype(F32)
    a_all[c] = (abar / emb_norm).astype(BF16)
    diag = INV_TEMP * jnp.sum(
        jnp.sum(img_u.astype(F32) * txt_u.astype(F32), axis=1, keepdims=True),
        axis=0, keepdims=True,
    )

    pl.semaphore_wait(barrier, 7 + 31 + 31)
    share(u_all, c, 0, row_peer, 8)
    share(t_all, r, 1, col_peer, 32)
    share(a_all, c, 2, row_peer, 8)

    arrived(u_all, 0, 8)
    arrived(t_all, 1, 32)
    img = u_all[...].astype(F32).reshape(64, 1024).astype(BF16)
    txt = t_all[...].astype(F32).reshape(256, 1024).astype(BF16)
    logits = INV_TEMP * dot(img, txt, NT)
    expo = jnp.exp(logits)
    cs_all[r] = jnp.sum(expo, axis=0, keepdims=True)
    share(cs_all, r, 3, col_peer, 32)
    rs_all[c] = pack_rows(jnp.sum(expo, axis=1, keepdims=True))
    share(rs_all, c, 4, row_peer, 8)
    arrived(rs_all, 4, 8)
    arrived(cs_all, 3, 32)

    row_tile = jnp.sum(rs_all[...], axis=0)
    rowsum = unpack_rows(row_tile)
    colsum = jnp.sum(cs_all[...], axis=0)
    probs = expo * (0.5 / rowsum + 0.5 / colsum)
    row = iota((64, 256), 0) - c * 8
    col = iota((64, 256), 1) - r * 8
    same = (row == col) & (row >= 0) & (row < 8)
    delta = (probs - jnp.where(same, 1.0, 0.0)).astype(BF16)
    s_part = jnp.sum(delta.astype(F32) * logits, axis=1, keepdims=True)
    own_rows = jnp.where(iota((8, 128), 1) == c, jnp.log(row_tile), 0.0)
    own = iota((1, 256), 1) - r * 8
    own_cols = jnp.where((own >= 0) & (own < 8), jnp.log(colsum), 0.0)
    loss = (
        jnp.sum(jnp.sum(own_rows, axis=1, keepdims=True), axis=0, keepdims=True)
        + jnp.sum(own_cols, axis=1, keepdims=True)
        - 2.0 * diag
    )
    s_tile = pack_rows(s_part)
    s_all[c] = jnp.where(iota((8, 128), 1) == 8, loss, s_tile)
    share(s_all, c, 5, row_peer, 8)
    grad = INV_TEMP * dot(delta, txt)
    for k in range(8):
        g_send[k] = grad[:, 128 * k : 128 * k + 128].astype(BF16)
    g_recv[c] = g_send[c]
    scatter(g_send, g_recv, c, 6, row_peer, 8)

    part = INV_TEMP * dot(probs.astype(BF16), img, TN)
    h_send[...] = part.astype(BF16).astype(F32).reshape(32, 8, 1024).astype(BF16)
    h_recv[r] = h_send[r]
    scatter(h_send, h_recv, r, 7, col_peer, 32)

    arrived(s_all, 5, 8)
    arrived(g_recv, 6, 8)
    arrived(a_all, 2, 8)
    s_sum = jnp.sum(s_all[...], axis=0)
    my_cols = pl.ds(pl.multiple_of(c * 128, 128), 128)
    f_cols = u_all[:, :, my_cols].astype(F32).reshape(64, 128)
    g_sum = jnp.sum(g_recv[...].astype(F32), axis=0)
    emb_grad = (g_sum - f_cols * unpack_rows(s_sum)).astype(BF16)
    scaled = a_all[...].astype(F32).reshape(64, 1024).astype(BF16)
    w_send[...] = dot(scaled, emb_grad, TN).astype(BF16).reshape(32, 32, 128)
    w_recv[r] = w_send[r]
    scatter(w_send, w_recv, r, 8, col_peer, 32)
    l_all[r] = jnp.sum(jnp.where(iota((8, 128), 1) == 8, s_sum, 0.0), axis=0, keepdims=True) * 0.125
    share(l_all, r, 9, col_peer, 32)

    arrived(w_recv, 8, 32)
    block = jnp.sum(w_recv[...].astype(F32), axis=0).astype(BF16)

    def chunk(a1, b1, core1):
        y1, x1 = place(a1, b1)
        return wgrad.at[
            pl.ds(pl.multiple_of(y1 * 256, 256), 256),
            pl.ds(pl.multiple_of((x1 * 2 + core1) * 128, 128), 128),
        ]

    mine = wgrad.at[pl.ds(pl.multiple_of(r * 32, 32), 32), my_cols]
    mine[...] = block

    def first(k, carry):
        pltpu.make_async_remote_copy(
            src_ref=mine, dst_ref=mine, send_sem=send.at[10], recv_sem=c1.at[a],
            device_id=plane_peer(k)[1], device_id_type=MESH,
        ).start()
        return carry

    lax.fori_loop(1, 32, first, 0)

    arrived(h_recv, 7, 32)
    g_txt = jnp.sum(h_recv[...].astype(F32), axis=0) - INV_TEMP * img_u.astype(F32)
    tgrad_ref[...] = (
        g_txt - txt_f * jnp.sum(txt_f * g_txt, axis=1, keepdims=True)
    ) / txt_norm
    arrived(l_all, 9, 32)
    total = jnp.sum(jnp.sum(l_all[...], axis=0), axis=1, keepdims=True)
    loss_ref[...] = jnp.broadcast_to(total * (1.0 / 4096.0), (1, 128))

    def second(j, carry):
        a1 = (a + j) % 4
        piece = chunk(a1, b, core)

        @pl.when(j == 0)
        def _():
            short = wgrad.at[pl.ds(0, 224), pl.ds(0, 128)]
            local(short, short, c1.at[a]).wait()

        @pl.when(j > 0)
        def _():
            local(piece, piece, c1.at[a1]).wait()

        for m in range(1, 4):
            pltpu.make_async_remote_copy(
                src_ref=piece, dst_ref=piece, send_sem=send.at[11],
                recv_sem=c2.at[b * 4 + a1],
                device_id=device(a, (b + m) % 4, z, core), device_id_type=MESH,
            ).start()
        pltpu.make_async_remote_copy(
            src_ref=piece, dst_ref=piece, send_sem=send.at[11], recv_sem=recv.at[10],
            device_id=(idx + 1 - 2 * core,), device_id_type=MESH,
        ).start()
        return carry

    lax.fori_loop(0, 4, second, 0)

    def third(t, carry):
        a1 = (a + t // 3) % 4
        b1 = (b + 1 + t % 3) % 4
        piece = chunk(a1, b1, core)
        local(piece, piece, c2.at[b1 * 4 + a1]).wait()
        pltpu.make_async_remote_copy(
            src_ref=piece, dst_ref=piece, send_sem=send.at[11], recv_sem=recv.at[10],
            device_id=(idx + 1 - 2 * core,), device_id_type=MESH,
        ).start()
        return carry

    lax.fori_loop(0, 12, third, 0)
    half = wgrad.at[:, pl.ds(0, 512)]
    local(half, half, recv.at[10]).wait()

    left(u_all, 0, 8)
    left(t_all, 1, 32)
    left(a_all, 2, 8)
    left(cs_all, 3, 32)
    left(rs_all, 4, 8)
    left(s_all, 5, 8)
    left(g_send, 6, 8)
    left(h_send, 7, 32)
    left(w_send, 8, 32)
    left(l_all, 9, 32)
    tall = wgrad.at[pl.ds(0, 992), pl.ds(0, 128)]
    local(tall, tall, send.at[10]).wait()
    wide = wgrad.at[:, pl.ds(0, 896)]
    local(wide, wide, send.at[11]).wait()


def contrast(emb, abar, text):
    images, width = emb.shape
    vmem = pl.BlockSpec(memory_space=pltpu.VMEM)
    return pl.pallas_call(
        loss_kernel,
        out_shape=[
            jax.ShapeDtypeStruct((width, width), BF16),
            jax.ShapeDtypeStruct((images, width), F32),
            jax.ShapeDtypeStruct((1, 128), F32),
        ],
        in_specs=[vmem, vmem, vmem],
        out_specs=[vmem, vmem, vmem],
        scratch_shapes=[
            pltpu.VMEM((32, 8, width), BF16),
            pltpu.VMEM((8, 8, width), BF16),
            pltpu.VMEM((8, 8, width), BF16),
            pltpu.VMEM((8, 8, 128), F32),
            pltpu.VMEM((32, 1, 256), F32),
            pltpu.VMEM((8, 64, 128), BF16),
            pltpu.VMEM((8, 64, 128), BF16),
            pltpu.VMEM((8, 8, 128), F32),
            pltpu.VMEM((32, 8, width), BF16),
            pltpu.VMEM((32, 8, width), BF16),
            pltpu.VMEM((32, 32, 128), BF16),
            pltpu.VMEM((32, 32, 128), BF16),
            pltpu.VMEM((32, 1, 128), F32),
            pltpu.SemaphoreType.DMA((12,)),
            pltpu.SemaphoreType.DMA((11,)),
            pltpu.SemaphoreType.DMA((4,)),
            pltpu.SemaphoreType.DMA((16,)),
        ],
        compiler_params=pltpu.CompilerParams(
            collective_id=0, has_side_effects=True, vmem_limit_bytes=40 << 20
        ),
        name="contrast",
    )(emb, abar, text)


def local(features, ln_gain, w_query, w_key, w_value, w_out, text_raw):
    emb, abar = embed(features, ln_gain.reshape(1, -1), w_query, w_key, w_value, w_out)
    wgrad, tgrad, loss = contrast(emb, abar, text_raw)
    return (loss[0, 0], tgrad, wgrad)


def solution(mesh):
    placed = (P("dp", None, None), P(), P(), P(), P(), P(), P("dp", None))
    return jax.shard_map(
        local, mesh=mesh, in_specs=placed, out_specs=(P(), P("dp", None), P()), check_vma=False
    )
```

```python
import jax
import jax.numpy as jnp
from jax import lax
from jax.experimental import pallas as pl
from jax.experimental.pallas import tpu as pltpu
from jax.sharding import PartitionSpec as P

INV_TEMP = 1.0 / 0.07
EPS = 1e-06
LOG2E = 1.4426950408889634
F32 = jnp.float32
BF16 = jnp.bfloat16
MESH = pl.DeviceIdType.MESH
NT = (((1,), (1,)), ((), ()))
TN = (((0,), (0,)), ((), ()))
NN = (((1,), (0,)), ((), ()))


def dot(a, b, dims=NN):
    return lax.dot_general(a, b, dims, preferred_element_type=F32)


def iota(shape, dim):
    return lax.broadcasted_iota(jnp.int32, shape, dim)


def pack_rows(col):
    lane = iota((8, 128), 1)
    tile = jnp.zeros((8, 128), F32)
    for k in range(8):
        tile = jnp.where(lane == k, col[8 * k : 8 * k + 8], tile)
    return tile


def unpack_rows(tile):
    return jnp.concatenate([tile[:, k : k + 1] for k in range(8)], axis=0)


def rows_of(ref):
    n, eight, width = ref.shape
    return ref[...].astype(F32).reshape(n * eight, width).astype(BF16)


def step_kernel(
    feat_hbm, gain_ref, wq_hbm, wk_hbm, wv_hbm, wo_hbm, text_ref,
    wgrad, tgrad_ref, loss_ref,
    feat, wq, wk, wv, wo, normed, qh, kh, vh, abar_f, xbar, fsem, wsem,
    t_all, t_row, u_all, u_col, a_all, rs_all, cs_all, rg_all, cg_all,
    g_send, g_recv, s_all, h_send, h_recv, w_send, w_recv, l_all, send, recv, c1, c2,
):
    idx = lax.axis_index("dp")
    core = idx % 2
    z = (idx // 2) % 8
    x = (idx // 16) % 4
    y = idx // 64
    c = x * 2 + core
    r = y * 8 + z

    def row_peer(k):
        p = (c + k) % 8
        return p, (y * 64 + (p // 2) * 16 + z * 2 + p % 2,)

    def col_peer(k):
        p = (r + k) % 32
        return p, ((p // 8) * 64 + x * 16 + (p % 8) * 2 + core,)

    a = y * (1 - core) + x * core
    b = x * (1 - core) + y * core

    def place(a1, b1):
        y1 = a1 * (1 - core) + b1 * core
        x1 = b1 * (1 - core) + a1 * core
        return y1, x1

    def device(a1, b1, z1, core1):
        y1, x1 = place(a1, b1)
        return (y1 * 64 + x1 * 16 + z1 * 2 + core1,)

    def plane_peer(k):
        p = (a * 8 + z + k) % 32
        return p, device(p // 8, b, p % 8, core)

    images = feat.shape[0]
    fcopy = [
        pltpu.make_async_copy(feat_hbm.at[i], feat.at[i], fsem.at[i]) for i in range(images)
    ]
    pairs = ((wq_hbm, wq), (wk_hbm, wk), (wv_hbm, wv), (wo_hbm, wo))
    wcopy = [pltpu.make_async_copy(s, d, wsem.at[i]) for i, (s, d) in enumerate(pairs)]
    for cp in fcopy + wcopy:
        cp.start()

    barrier = pltpu.get_barrier_semaphore()

    def greet(peer):
        def step(k, carry):
            pl.semaphore_signal(barrier, inc=1, device_id=peer(k)[1], device_id_type=MESH)
            return carry

        return step

    lax.fori_loop(1, 8, greet(row_peer), 0)
    lax.fori_loop(1, 32, greet(col_peer), 0)
    lax.fori_loop(1, 32, greet(plane_peer), 0)

    def push(src, dst, s, dev):
        pltpu.make_async_remote_copy(
            src_ref=src, dst_ref=dst, send_sem=send.at[s], recv_sem=recv.at[s],
            device_id=dev, device_id_type=MESH,
        ).start()

    def share(buf, slot, s, peer, n):
        def step(k, carry):
            push(buf.at[slot], buf.at[slot], s, peer(k)[1])
            return carry

        lax.fori_loop(1, n, step, 0)

    def scatter(src, dst, slot, s, peer, n):
        def step(k, carry):
            p, dev = peer(k)
            push(src.at[p], dst.at[slot], s, dev)
            return carry

        lax.fori_loop(1, n, step, 0)

    def local(src, dst, sem):
        return pltpu.make_async_copy(src, dst, sem)

    def arrived(buf, s, n):
        part = buf.at[pl.ds(0, n - 1)]
        local(part, part, recv.at[s]).wait()

    def left(buf, s, n):
        part = buf.at[pl.ds(0, n - 1)]
        local(part, part, send.at[s]).wait()

    text = text_ref[...].astype(F32)
    txt_norm = jnp.sqrt(jnp.sum(text * text, axis=1, keepdims=True) + EPS)
    txt_f = text / txt_norm
    txt_u = txt_f.astype(BF16)
    t_all[r] = txt_u
    t_row[c] = txt_u
    gain = gain_ref[...]

    with jax.named_scope("norm"):
        for i in range(images):
            fcopy[i].wait()

            def norm_rows(t, total, i=i):
                rows = pl.ds(pl.multiple_of(t * 32, 32), 32)
                x = feat[i, rows, :].astype(F32)
                center = x - jnp.mean(x, axis=-1, keepdims=True)
                spread = jnp.mean(center * center, axis=-1, keepdims=True)
                out = center * lax.rsqrt(spread + EPS) * gain
                normed[pl.ds(pl.multiple_of(i * 128 + t * 32, 32), 32), :] = out.astype(BF16)
                return total + jnp.sum(x.reshape(4, 8, 1024), axis=0)

            total = lax.fori_loop(0, 4, norm_rows, jnp.zeros((8, 1024), F32))
            total = jnp.sum(total, axis=0, keepdims=True)
            first = feat[i, 0:16, :].astype(F32)[0:1]
            xbar[i : i + 1, :] = first + (total - first) * (1.0 / 127.0)

    with jax.named_scope("greet"):
        pl.semaphore_wait(barrier, 7 + 31 + 31)
        share(t_all, r, 1, col_peer, 32)
        share(t_row, c, 12, row_peer, 8)

    same_head = jnp.where(
        iota((256, 256), 0) // 64 == iota((256, 256), 1) // 64, 1.0, 0.0
    ).astype(BF16)

    def project(w, out, scale):
        def step(t, carry):
            rows = pl.ds(pl.multiple_of((t % 2) * 512, 512), 512)
            cols = pl.ds(pl.multiple_of((t // 2) * 256, 256), 256)
            proj = dot(normed[rows, :], w[:, cols])
            if scale is not None:
                squares = dot((proj * proj).astype(BF16), same_head)
                proj = proj * (lax.rsqrt(squares + EPS) * scale)
            out[rows, cols] = proj.astype(BF16)
            return carry

        lax.fori_loop(0, 8, step, 0)

    with jax.named_scope("query"):
        wcopy[0].wait()
        project(wq, qh, 8.0 * LOG2E)
    with jax.named_scope("key"):
        wcopy[1].wait()
        project(wk, kh, 1.0)
    with jax.named_scope("value"):
        wcopy[2].wait()
        project(wv, vh, None)

    lane = iota((1, 128), 1)
    low = jnp.where(lane < 64, 1.0, 0.0).astype(BF16)
    high = jnp.where(lane < 64, 0.0, 1.0).astype(BF16)
    weigh = jnp.where(iota((1, 256), 1) % 128 == 0, 1.0, 1.0 / 127.0).astype(F32)
    gather = jnp.where(
        iota((256, 128), 0) // 128 == iota((256, 128), 1) // 64, 1.0, 0.0
    ).astype(BF16)

    def attend(i, carry):
        rows = pl.ds(pl.multiple_of(i * 128, 128), 128)
        parts = []
        for p in range(8):
            cols = slice(p * 128, p * 128 + 128)
            q = qh[rows, cols]
            both = jnp.concatenate([q * low, q * high], axis=0)
            expo = jnp.exp2(dot(kh[rows, cols], both, NT))
            weight = weigh / jnp.sum(expo, axis=0, keepdims=True)
            pooled = dot((expo * weight).astype(BF16), gather)
            parts.append(jnp.sum(pooled * vh[rows, cols].astype(F32), axis=0, keepdims=True))
        abar_f[pl.ds(i, 1), :] = jnp.concatenate(parts, axis=1)
        return carry

    with jax.named_scope("attend"):
        lax.fori_loop(0, images, attend, 0)

    with jax.named_scope("emb"):
        abar = abar_f[...].astype(BF16)
        wcopy[3].wait()
        emb = xbar[...] + dot(abar, wo[...])
        emb_norm = jnp.sqrt(jnp.sum(emb * emb, axis=1, keepdims=True) + EPS)
        img_u = (emb / emb_norm).astype(BF16)
        u_all[c] = img_u
        u_col[r] = img_u
        a_all[c] = (abar.astype(F32) / emb_norm).astype(BF16)
        share(u_all, c, 0, row_peer, 8)
        share(a_all, c, 2, row_peer, 8)
        diag = INV_TEMP * jnp.sum(
            jnp.sum(img_u.astype(F32) * txt_u.astype(F32), axis=1, keepdims=True),
            axis=0, keepdims=True,
        )

    with jax.named_scope("wait_text"):
        arrived(t_all, 1, 32)
    with jax.named_scope("wait_img"):
        arrived(u_all, 0, 8)
    with jax.named_scope("logits"):
        img = rows_of(u_all)
        txt = rows_of(t_all)
        logits = INV_TEMP * dot(img, txt, NT)
        expo = jnp.exp(logits)
        cs_all[r] = jnp.sum(expo, axis=0, keepdims=True)
        share(cs_all, r, 3, col_peer, 32)
        rs_all[c] = pack_rows(jnp.sum(expo, axis=1, keepdims=True))
        share(rs_all, c, 4, row_peer, 8)
        share(u_col, r, 13, col_peer, 32)
    with jax.named_scope("wait_sums"):
        arrived(rs_all, 4, 8)
        arrived(cs_all, 3, 32)

    with jax.named_scope("delta"):
        row_tile = jnp.sum(rs_all[...], axis=0)
        colsum = jnp.sum(cs_all[...], axis=0)
        probs = expo * (0.5 / unpack_rows(row_tile) + 0.5 / colsum)
        row = iota((64, 256), 0) - c * 8
        col = iota((64, 256), 1) - r * 8
        same = (row == col) & (row >= 0) & (row < 8)
        delta = (probs - jnp.where(same, 1.0, 0.0)).astype(BF16)
        grad = INV_TEMP * dot(delta, txt)
        for k in range(8):
            g_send[k] = grad[:, 128 * k : 128 * k + 128].astype(BF16)
        g_recv[c] = g_send[c]
        scatter(g_send, g_recv, c, 6, row_peer, 8)
        s_part = jnp.sum(delta.astype(F32) * logits, axis=1, keepdims=True)
        my_lane = iota((8, 128), 1) == c
        own_rows = jnp.where(my_lane, row_tile, 0.0)
        own = iota((1, 256), 1) - r * 8
        own_cols = jnp.where((own >= 0) & (own < 8), colsum, 0.0)
        loss = (
            jnp.sum(
                jnp.sum(jnp.log(jnp.where(my_lane, row_tile, 1.0)), axis=1, keepdims=True),
                axis=0, keepdims=True,
            )
            + jnp.sum(
                jnp.log(jnp.where((own >= 0) & (own < 8), colsum, 1.0)), axis=1, keepdims=True
            )
            - 2.0 * diag
        )
        s_all[c] = jnp.where(iota((8, 128), 1) == 8, loss, pack_rows(s_part))
        share(s_all, c, 5, row_peer, 8)
        own_row = jnp.sum(own_rows, axis=1, keepdims=True)
        spot = iota((8, 256), 1) - r * 8 == iota((8, 256), 0)
        rg_all[r] = jnp.sum(jnp.where(spot, own_row, 0.0), axis=0, keepdims=True)
        share(rg_all, r, 14, col_peer, 32)
        own_col = jnp.sum(jnp.where(spot, own_cols, 0.0), axis=1, keepdims=True)
        cg_all[c] = jnp.where(my_lane, own_col, 0.0)
        share(cg_all, c, 15, row_peer, 8)

    with jax.named_scope("wait_grad"):
        arrived(s_all, 5, 8)
        arrived(g_recv, 6, 8)
        arrived(a_all, 2, 8)
    with jax.named_scope("wgrad"):
        s_sum = jnp.sum(s_all[...], axis=0)
        my_cols = pl.ds(pl.multiple_of(c * 128, 128), 128)
        f_cols = u_all[:, :, my_cols].astype(F32).reshape(64, 128)
        g_sum = jnp.sum(g_recv[...].astype(F32), axis=0)
        emb_grad = (g_sum - f_cols * unpack_rows(s_sum)).astype(BF16)
        w_send[...] = dot(rows_of(a_all), emb_grad, TN).astype(BF16).reshape(32, 32, 128)
        w_recv[r] = w_send[r]
        scatter(w_send, w_recv, r, 8, col_peer, 32)
        l_all[r] = (
            jnp.sum(jnp.where(iota((8, 128), 1) == 8, s_sum, 0.0), axis=0, keepdims=True) * 0.125
        )
        share(l_all, r, 9, col_peer, 32)

    with jax.named_scope("wait_bulk"):
        arrived(u_col, 13, 32)
        arrived(t_row, 12, 8)
        arrived(rg_all, 14, 32)
        arrived(cg_all, 15, 8)
    with jax.named_scope("text"):
        every = rows_of(u_col)
        expo_t = jnp.exp(INV_TEMP * dot(rows_of(t_row), every, NT))
        rowsum_t = jnp.sum(rg_all[...], axis=0)
        colsum_t = unpack_rows(jnp.sum(cg_all[...], axis=0))
        probs_t = (expo_t * (0.5 / colsum_t + 0.5 / rowsum_t)).astype(BF16)
        h_send[...] = (INV_TEMP * dot(probs_t, every)).reshape(8, 8, 1024)
        h_recv[c] = h_send[c]
        scatter(h_send, h_recv, c, 7, row_peer, 8)

    with jax.named_scope("wait_w"):
        arrived(w_recv, 8, 32)

    def chunk(a1, b1, core1):
        y1, x1 = place(a1, b1)
        return wgrad.at[
            pl.ds(pl.multiple_of(y1 * 256, 256), 256),
            pl.ds(pl.multiple_of((x1 * 2 + core1) * 128, 128), 128),
        ]

    with jax.named_scope("first"):
        mine = wgrad.at[pl.ds(pl.multiple_of(r * 32, 32), 32), my_cols]
        mine[...] = jnp.sum(w_recv[...].astype(F32), axis=0).astype(BF16)

        def first(k, carry):
            pltpu.make_async_remote_copy(
                src_ref=mine, dst_ref=mine, send_sem=send.at[10], recv_sem=c1.at[a],
                device_id=plane_peer(k)[1], device_id_type=MESH,
            ).start()
            return carry

        lax.fori_loop(1, 32, first, 0)

    partner = (idx + 1 - 2 * core,)

    def forward(piece):
        pltpu.make_async_remote_copy(
            src_ref=piece, dst_ref=piece, send_sem=send.at[11], recv_sem=recv.at[10],
            device_id=partner, device_id_type=MESH,
        ).start()

    def second(j, carry):
        a1 = (a + j) % 4
        piece = chunk(a1, b, core)

        @pl.when(j == 0)
        def _():
            short = wgrad.at[pl.ds(0, 224), pl.ds(0, 128)]
            local(short, short, c1.at[a]).wait()

        @pl.when(j > 0)
        def _():
            local(piece, piece, c1.at[a1]).wait()

        for m in range(1, 4):
            pltpu.make_async_remote_copy(
                src_ref=piece, dst_ref=piece, send_sem=send.at[11],
                recv_sem=c2.at[b * 4 + a1],
                device_id=device(a, (b + m) % 4, z, core), device_id_type=MESH,
            ).start()
        forward(piece)
        return carry

    with jax.named_scope("second"):
        lax.fori_loop(0, 4, second, 0)

    def third(t, carry):
        a1 = (a + t // 3) % 4
        b1 = (b + 1 + t % 3) % 4
        piece = chunk(a1, b1, core)
        local(piece, piece, c2.at[b1 * 4 + a1]).wait()
        forward(piece)
        return carry

    with jax.named_scope("third"):
        lax.fori_loop(0, 12, third, 0)

    with jax.named_scope("text_out"):
        arrived(h_recv, 7, 8)
        g_txt = jnp.sum(h_recv[...], axis=0) - INV_TEMP * img_u.astype(F32)
        tgrad_ref[...] = (
            g_txt - txt_f * jnp.sum(txt_f * g_txt, axis=1, keepdims=True)
        ) / txt_norm
        arrived(l_all, 9, 32)
        total = jnp.sum(jnp.sum(l_all[...], axis=0), axis=1, keepdims=True)
        loss_ref[...] = jnp.broadcast_to(total * (1.0 / 4096.0), (1, 128))

    with jax.named_scope("drain"):
        half = wgrad.at[:, pl.ds(0, 512)]
        local(half, half, recv.at[10]).wait()
        left(u_all, 0, 8)
        left(t_all, 1, 32)
        left(a_all, 2, 8)
        left(cs_all, 3, 32)
        left(rs_all, 4, 8)
        left(s_all, 5, 8)
        left(g_send, 6, 8)
        left(h_send, 7, 8)
        left(w_send, 8, 32)
        left(l_all, 9, 32)
        left(t_row, 12, 8)
        left(u_col, 13, 32)
        left(rg_all, 14, 32)
        left(cg_all, 15, 8)
        tall = wgrad.at[pl.ds(0, 992), pl.ds(0, 128)]
        local(tall, tall, send.at[10]).wait()
        wide = wgrad.at[:, pl.ds(0, 896)]
        local(wide, wide, send.at[11]).wait()


def step(features, gain, wq, wk, wv, wo, text):
    images, tokens, width = features.shape
    rows = images * tokens
    hbm = pl.BlockSpec(memory_space=pltpu.HBM)
    vmem = pl.BlockSpec(memory_space=pltpu.VMEM)
    return pl.pallas_call(
        step_kernel,
        out_shape=[
            jax.ShapeDtypeStruct((width, width), BF16),
            jax.ShapeDtypeStruct((images, width), F32),
            jax.ShapeDtypeStruct((1, 128), F32),
        ],
        in_specs=[hbm, vmem, hbm, hbm, hbm, hbm, vmem],
        out_specs=[vmem, vmem, vmem],
        scratch_shapes=[
            pltpu.VMEM((images, tokens, width), BF16),
            *[pltpu.VMEM((width, width), BF16)] * 4,
            *[pltpu.VMEM((rows, width), BF16)] * 4,
            pltpu.VMEM((images, width), F32),
            pltpu.VMEM((images, width), F32),
            pltpu.SemaphoreType.DMA((images,)),
            pltpu.SemaphoreType.DMA((4,)),
            pltpu.VMEM((32, 8, width), BF16),
            pltpu.VMEM((8, 8, width), BF16),
            pltpu.VMEM((8, 8, width), BF16),
            pltpu.VMEM((32, 8, width), BF16),
            pltpu.VMEM((8, 8, width), BF16),
            pltpu.VMEM((8, 8, 128), F32),
            pltpu.VMEM((32, 1, 256), F32),
            pltpu.VMEM((32, 1, 256), F32),
            pltpu.VMEM((8, 8, 128), F32),
            pltpu.VMEM((8, 64, 128), BF16),
            pltpu.VMEM((8, 64, 128), BF16),
            pltpu.VMEM((8, 8, 128), F32),
            pltpu.VMEM((8, 8, width), F32),
            pltpu.VMEM((8, 8, width), F32),
            pltpu.VMEM((32, 32, 128), BF16),
            pltpu.VMEM((32, 32, 128), BF16),
            pltpu.VMEM((32, 1, 128), F32),
            pltpu.SemaphoreType.DMA((16,)),
            pltpu.SemaphoreType.DMA((16,)),
            pltpu.SemaphoreType.DMA((4,)),
            pltpu.SemaphoreType.DMA((16,)),
        ],
        compiler_params=pltpu.CompilerParams(
            collective_id=0, has_side_effects=True, vmem_limit_bytes=64 * 1024 * 1000
        ),
        name="step",
    )(features, gain, wq, wk, wv, wo, text)


def whole(features, ln_gain, w_query, w_key, w_value, w_out, text_raw):
    wgrad, tgrad, loss = step(
        features, ln_gain.reshape(1, -1), w_query, w_key, w_value, w_out, text_raw
    )
    return (loss[0, 0], tgrad, wgrad)


def solution(mesh):
    placed = (P("dp", None, None), P(), P(), P(), P(), P(), P("dp", None))
    return jax.shard_map(
        whole, mesh=mesh, in_specs=placed, out_specs=(P(), P("dp", None), P()), check_vma=False
    )
```

```python
import jax
import jax.numpy as jnp
from jax import lax
from jax.experimental import pallas as pl
from jax.experimental.pallas import tpu as pltpu
from jax.sharding import PartitionSpec as P

INV_TEMP = 1.0 / 0.07
EPS = 1e-06
LOG2E = 1.4426950408889634
F32 = jnp.float32
BF16 = jnp.bfloat16
MESH = pl.DeviceIdType.MESH
NT = (((1,), (1,)), ((), ()))
TN = (((0,), (0,)), ((), ()))
NN = (((1,), (0,)), ((), ()))


def dot(a, b, dims=NN):
    return lax.dot_general(a, b, dims, preferred_element_type=F32)


def iota(shape, dim):
    return lax.broadcasted_iota(jnp.int32, shape, dim)


def pack_rows(col):
    lane = iota((8, 128), 1)
    tile = jnp.zeros((8, 128), F32)
    for k in range(8):
        tile = jnp.where(lane == k, col[8 * k : 8 * k + 8], tile)
    return tile


def unpack_rows(tile):
    return jnp.concatenate([tile[:, k : k + 1] for k in range(8)], axis=0)


def rows_of(ref):
    n, eight, width = ref.shape
    return ref[...].astype(F32).reshape(n * eight, width).astype(BF16)


def step_kernel(
    feat_hbm, gain_hbm, wq_hbm, wk_hbm, wv_hbm, wo_hbm, text_hbm,
    wgrad, tgrad_ref, loss_ref,
    feat, wq, wk, wv, wo, normed, qh, kh, vh, abar_f, xbar, gain_v, text_v, fsem, wsem,
    t_all, t_row, u_all, u_col, a_all, rs_all, cs_all, rg_all, cg_all,
    g_send, g_recv, s_all, h_send, h_recv, w_send, w_recv, l_all, send, recv, c1, c2,
):
    div, rem = lax.div, lax.rem
    idx = lax.axis_index("dp")
    core = rem(idx, 2)
    z = rem(div(idx, 2), 8)
    x = rem(div(idx, 16), 4)
    y = div(idx, 64)
    c = x * 2 + core
    r = y * 8 + z
    q = div(idx, 16) * 2 + core

    def row_peer(k):
        p = rem(c + k, 8)
        return p, (y * 64 + div(p, 2) * 16 + z * 2 + rem(p, 2),)

    def col_peer(k):
        p = rem(r + k, 32)
        return p, (div(p, 8) * 64 + x * 16 + rem(p, 8) * 2 + core,)

    def ring_peer(k):
        p = rem(z + k, 8)
        return p, (idx + (p - z) * 2,)

    def side_peer(k):
        p = rem(q + k, 32)
        return p, (div(p, 2) * 16 + z * 2 + rem(p, 2),)

    a = y * (1 - core) + x * core
    b = x * (1 - core) + y * core

    def place(a1, b1):
        y1 = a1 * (1 - core) + b1 * core
        x1 = b1 * (1 - core) + a1 * core
        return y1, x1

    def device(a1, b1, z1, core1):
        y1, x1 = place(a1, b1)
        return (y1 * 64 + x1 * 16 + z1 * 2 + core1,)

    def plane_peer(k):
        p = rem(a * 8 + z + k, 32)
        return p, device(div(p, 8), b, rem(p, 8), core)

    def b_peer(k):
        return rem(b + k, 4), device(a, rem(b + k, 4), z, core)

    partner = (idx + 1 - 2 * core,)

    images = feat.shape[0]
    fcopy = [
        pltpu.make_async_copy(feat_hbm.at[i], feat.at[i], fsem.at[i]) for i in range(images)
    ]
    pairs = ((wq_hbm, wq), (wk_hbm, wk), (wv_hbm, wv), (wo_hbm, wo))
    wcopy = [pltpu.make_async_copy(s, d, wsem.at[i]) for i, (s, d) in enumerate(pairs)]
    gcopy = pltpu.make_async_copy(gain_hbm, gain_v, wsem.at[4])
    tcopy = pltpu.make_async_copy(text_hbm, text_v, wsem.at[5])
    for cp in [gcopy, *fcopy, *wcopy, tcopy]:
        cp.start()

    barrier = pltpu.get_barrier_semaphore()

    def greet(peer):
        def step(k, carry):
            pl.semaphore_signal(barrier, inc=1, device_id=peer(k)[1], device_id_type=MESH)
            return carry

        return step

    lax.fori_loop(1, 32, greet(col_peer), 0, unroll=True)
    lax.fori_loop(1, 32, greet(side_peer), 0, unroll=True)
    lax.fori_loop(1, 32, greet(plane_peer), 0, unroll=True)

    def push(src, dst, s, dev):
        pltpu.make_async_remote_copy(
            src_ref=src, dst_ref=dst, send_sem=send.at[s], recv_sem=recv.at[s],
            device_id=dev, device_id_type=MESH,
        ).start()

    def share(buf, slot, s, peer, n):
        def step(k, carry):
            push(buf.at[slot], buf.at[slot], s, peer(k)[1])
            return carry

        lax.fori_loop(1, n, step, 0, unroll=True)

    def scatter(src, dst, slot, s, peer, n):
        def step(k, carry):
            p, dev = peer(k)
            push(src.at[p], dst.at[slot], s, dev)
            return carry

        lax.fori_loop(1, n, step, 0, unroll=True)

    def local(src, dst, sem):
        return pltpu.make_async_copy(src, dst, sem)

    def arrived(buf, s, n):
        part = buf.at[pl.ds(0, n - 1)]
        local(part, part, recv.at[s]).wait()

    def left(buf, s, n):
        part = buf.at[pl.ds(0, n - 1)]
        local(part, part, send.at[s]).wait()

    gcopy.wait()
    gain = gain_v[...]

    with jax.named_scope("norm"):
        for i in range(images):
            fcopy[i].wait()

            total = jnp.zeros((8, 1024), F32)
            for t in range(2):
                rows = slice(t * 64, t * 64 + 64)
                tok = feat[i, rows, :].astype(F32)
                center = tok - jnp.mean(tok, axis=-1, keepdims=True)
                spread = jnp.mean(center * center, axis=-1, keepdims=True)
                out = center * lax.rsqrt(spread + EPS) * gain
                normed[i * 128 + t * 64 : i * 128 + t * 64 + 64, :] = out.astype(BF16)
                total = total + jnp.sum(tok.reshape(8, 8, 1024), axis=0)
            total = jnp.sum(total, axis=0, keepdims=True)
            first = feat[i, 0:16, :].astype(F32)[0:1]
            xbar[i : i + 1, :] = first + (total - first) * (1.0 / 127.0)

    same_head = jnp.where(
        iota((256, 256), 0) // 64 == iota((256, 256), 1) // 64, 1.0, 0.0
    ).astype(BF16)

    def unit(proj, scale):
        squares = dot((proj * proj).astype(BF16), same_head)
        return (proj * (lax.rsqrt(squares + EPS) * scale)).astype(BF16)

    def project(t, carry):
        cols = pl.ds(pl.multiple_of(t * 256, 256), 256)
        tokens = normed[...]
        query = dot(tokens, wq[:, cols])
        key = dot(tokens, wk[:, cols])
        qh[:, cols] = unit(query, 8.0 * LOG2E)
        kh[:, cols] = unit(key, 1.0)
        vh[:, cols] = dot(tokens, wv[:, cols]).astype(BF16)
        return carry

    with jax.named_scope("greet"):
        tcopy.wait()
        text = text_v[...].astype(F32)
        txt_norm = jnp.sqrt(jnp.sum(text * text, axis=1, keepdims=True) + EPS)
        txt_f = text / txt_norm
        txt_u = txt_f.astype(BF16)
        t_all[r] = txt_u
        t_row[z] = txt_u
        pl.semaphore_wait(barrier, 31 + 31 + 31)
        share(t_all, r, 1, col_peer, 32)
        share(t_row, z, 12, ring_peer, 8)

    with jax.named_scope("project"):
        for i in range(3):
            wcopy[i].wait()
        lax.fori_loop(0, 4, project, 0)

    lane = iota((1, 128), 1)
    low = jnp.where(lane < 64, 1.0, 0.0).astype(BF16)
    high = jnp.where(lane < 64, 0.0, 1.0).astype(BF16)
    weigh = jnp.where(iota((1, 256), 1) % 128 == 0, 1.0, 1.0 / 127.0).astype(F32)
    gather = jnp.where(
        iota((256, 128), 0) // 128 == iota((256, 128), 1) // 64, 1.0, 0.0
    ).astype(BF16)

    def attend(i, carry):
        rows = pl.ds(pl.multiple_of(i * 128, 128), 128)
        parts = []
        for p in range(8):
            cols = slice(p * 128, p * 128 + 128)
            q = qh[rows, cols]
            both = jnp.concatenate([q * low, q * high], axis=0)
            expo = jnp.exp2(dot(kh[rows, cols], both, NT))
            weight = weigh / jnp.sum(expo, axis=0, keepdims=True)
            parts.append((expo * weight).astype(BF16))
        pooled = dot(jnp.concatenate(parts, axis=0), gather)
        sums = []
        for p in range(8):
            value = vh[rows, p * 128 : p * 128 + 128].astype(F32)
            sums.append(
                jnp.sum(pooled[p * 128 : p * 128 + 128] * value, axis=0, keepdims=True)
            )
        abar_f[pl.ds(i, 1), :] = jnp.concatenate(sums, axis=1)
        return carry

    with jax.named_scope("attend"):
        lax.fori_loop(0, images, attend, 0)

    with jax.named_scope("emb"):
        abar = abar_f[...].astype(BF16)
        wcopy[3].wait()
        emb = xbar[...] + dot(abar, wo[...])
        emb_norm = jnp.sqrt(jnp.sum(emb * emb, axis=1, keepdims=True) + EPS)
        img_u = (emb / emb_norm).astype(BF16)
        u_all[c] = img_u
        u_col[q] = img_u
        a_all[c] = (abar.astype(F32) / emb_norm).astype(BF16)
        share(u_all, c, 0, row_peer, 8)
        share(a_all, c, 2, row_peer, 8)
        diag = INV_TEMP * jnp.sum(
            jnp.sum(img_u.astype(F32) * txt_u.astype(F32), axis=1, keepdims=True),
            axis=0, keepdims=True,
        )

    with jax.named_scope("wait_text"):
        arrived(t_all, 1, 32)
    with jax.named_scope("wait_img"):
        arrived(u_all, 0, 8)
    with jax.named_scope("logits"):
        img = rows_of(u_all)
        txt = rows_of(t_all)
        logits = INV_TEMP * dot(img, txt, NT)
        expo = jnp.exp(logits)
        cs_all[r] = jnp.sum(expo, axis=0, keepdims=True)
        share(cs_all, r, 3, col_peer, 32)
        rs_all[c] = pack_rows(jnp.sum(expo, axis=1, keepdims=True))
        share(rs_all, c, 4, row_peer, 8)
        share(u_col, q, 13, side_peer, 32)
    with jax.named_scope("wait_sums"):
        arrived(rs_all, 4, 8)
        arrived(cs_all, 3, 32)

    with jax.named_scope("delta"):
        row_tile = jnp.sum(rs_all[...], axis=0)
        colsum = jnp.sum(cs_all[...], axis=0)
        probs = expo * (0.5 / unpack_rows(row_tile) + 0.5 / colsum)
        row = iota((64, 256), 0) - c * 8
        col = iota((64, 256), 1) - r * 8
        same = (row == col) & (row >= 0) & (row < 8)
        delta = (probs - jnp.where(same, 1.0, 0.0)).astype(BF16)
        grad = INV_TEMP * dot(delta, txt)
        for k in range(8):
            g_send[k] = grad[:, 128 * k : 128 * k + 128].astype(BF16)
        g_recv[c] = g_send[c]
        scatter(g_send, g_recv, c, 6, row_peer, 8)
        s_part = jnp.sum(delta.astype(F32) * logits, axis=1, keepdims=True)
        my_lane = iota((8, 128), 1) == c
        own_rows = jnp.where(my_lane, row_tile, 0.0)
        own = iota((1, 256), 1) - r * 8
        own_cols = jnp.where((own >= 0) & (own < 8), colsum, 0.0)
        loss = (
            jnp.sum(
                jnp.sum(jnp.log(jnp.where(my_lane, row_tile, 1.0)), axis=1, keepdims=True),
                axis=0, keepdims=True,
            )
            + jnp.sum(
                jnp.log(jnp.where((own >= 0) & (own < 8), colsum, 1.0)), axis=1, keepdims=True
            )
            - 2.0 * diag
        )
        s_all[c] = jnp.where(iota((8, 128), 1) == 8, loss, pack_rows(s_part))
        share(s_all, c, 5, row_peer, 8)
        own_row = jnp.sum(own_rows, axis=1, keepdims=True)
        spot = iota((8, 256), 1) - iota((8, 256), 0)
        rg_all[q] = jnp.sum(jnp.where(spot == q * 8, own_row, 0.0), axis=0, keepdims=True)
        share(rg_all, q, 14, side_peer, 32)
        own_col = jnp.sum(jnp.where(spot == r * 8, own_cols, 0.0), axis=1, keepdims=True)
        cg_all[z] = jnp.where(iota((8, 128), 1) == z, own_col, 0.0)
        share(cg_all, z, 15, ring_peer, 8)

    with jax.named_scope("wait_grad"):
        arrived(s_all, 5, 8)
        arrived(g_recv, 6, 8)
        arrived(a_all, 2, 8)
    with jax.named_scope("wgrad"):
        s_sum = jnp.sum(s_all[...], axis=0)
        my_cols = pl.ds(pl.multiple_of(c * 128, 128), 128)
        f_cols = u_all[:, :, my_cols].astype(F32).reshape(64, 128)
        g_sum = jnp.sum(g_recv[...].astype(F32), axis=0)
        emb_grad = (g_sum - f_cols * unpack_rows(s_sum)).astype(BF16)
        w_send[...] = dot(rows_of(a_all), emb_grad, TN).astype(BF16).reshape(32, 32, 128)
        w_recv[r] = w_send[r]
        scatter(w_send, w_recv, r, 8, col_peer, 32)
        l_all[r] = (
            jnp.sum(jnp.where(iota((8, 128), 1) == 8, s_sum, 0.0), axis=0, keepdims=True) * 0.125
        )
        share(l_all, r, 9, col_peer, 32)

    with jax.named_scope("wait_bulk"):
        arrived(u_col, 13, 32)
        arrived(t_row, 12, 8)
        arrived(rg_all, 14, 32)
        arrived(cg_all, 15, 8)
    with jax.named_scope("text"):
        every = rows_of(u_col)
        expo_t = jnp.exp(INV_TEMP * dot(rows_of(t_row), every, NT))
        rowsum_t = jnp.sum(rg_all[...], axis=0)
        colsum_t = unpack_rows(jnp.sum(cg_all[...], axis=0))
        probs_t = (expo_t * (0.5 / colsum_t + 0.5 / rowsum_t)).astype(BF16)
        h_send[...] = (INV_TEMP * dot(probs_t, every)).reshape(8, 8, 1024).astype(BF16)
        h_recv[z] = h_send[z]

    with jax.named_scope("wait_w"):
        arrived(w_recv, 8, 32)

    def part(a1, b1, first, size):
        y1, x1 = place(a1, b1)
        return wgrad.at[
            pl.ds(pl.multiple_of(y1 * 256 + first, 32), size),
            pl.ds(pl.multiple_of((x1 * 2 + core) * 128, 128), 128),
        ]

    def block(a1, b1, z1):
        return part(a1, b1, z1 * 32, 32)

    def chunk(a1, b1):
        return part(a1, b1, 0, 256)

    def pass_on(piece, s, arrival, dev):
        pltpu.make_async_remote_copy(
            src_ref=piece, dst_ref=piece, send_sem=send.at[s], recv_sem=arrival,
            device_id=dev, device_id_type=MESH,
        ).start()

    def to_b(piece, a1):
        for m in (2, 1, 3):
            pass_on(piece, 11, c2.at[b * 4 + a1], b_peer(m)[1])

    order = sorted(
        [(i, j) for i in range(4) for j in range(8) if i or j],
        key=lambda t: (min(t[1], 8 - t[1]) + min(t[0], 4 - t[0]), t),
    )

    with jax.named_scope("first"):
        mine = block(a, b, z)
        mine[...] = jnp.sum(w_recv[...].astype(F32), axis=0).astype(BF16)
        for i, j in order:
            pass_on(mine, 10, c1.at[a * 8 + z], device(rem(a + i, 4), b, rem(z + j, 8), core))
        to_b(mine, a)

    with jax.named_scope("second"):
        for i, j in order:
            a1, z1 = rem(a + 4 - i, 4), rem(z + 8 - j, 8)
            piece = block(a1, b, z1)
            local(piece, piece, c1.at[a1 * 8 + z1]).wait()
            to_b(piece, a1)
        for k in range(4):
            pass_on(chunk(rem(a + k, 4), b), 11, recv.at[10], partner)
        scatter(h_send, h_recv, z, 7, ring_peer, 8)

    def fourth(t, carry):
        a1, b1 = rem(a + div(t, 3), 4), rem(b + 1 + rem(t, 3), 4)
        piece = chunk(a1, b1)
        local(piece, piece, c2.at[b1 * 4 + a1]).wait()
        pass_on(piece, 11, recv.at[10], partner)
        return carry

    with jax.named_scope("fourth"):
        lax.fori_loop(0, 12, fourth, 0)

    with jax.named_scope("text_out"):
        arrived(h_recv, 7, 8)
        g_txt = jnp.sum(h_recv[...].astype(F32), axis=0) - INV_TEMP * img_u.astype(F32)
        tgrad_ref[...] = (
            g_txt - txt_f * jnp.sum(txt_f * g_txt, axis=1, keepdims=True)
        ) / txt_norm
        arrived(l_all, 9, 32)
        total = jnp.sum(jnp.sum(l_all[...], axis=0), axis=1, keepdims=True)
        loss_ref[...] = jnp.broadcast_to(total * (1.0 / 4096.0), (1, 128))

    with jax.named_scope("drain"):
        half = wgrad.at[pl.ds(0, 512)]
        local(half, half, recv.at[10]).wait()
        left(u_all, 0, 8)
        left(t_all, 1, 32)
        left(a_all, 2, 8)
        left(cs_all, 3, 32)
        left(rs_all, 4, 8)
        left(s_all, 5, 8)
        left(g_send, 6, 8)
        left(h_send, 7, 8)
        left(w_send, 8, 32)
        left(l_all, 9, 32)
        left(t_row, 12, 8)
        left(u_col, 13, 32)
        left(rg_all, 14, 32)
        left(cg_all, 15, 8)
        tall = wgrad.at[pl.ds(0, 992), pl.ds(0, 128)]
        local(tall, tall, send.at[10]).wait()
        wide = wgrad.at[pl.ds(0, 896)]
        local(wide, wide, send.at[11]).wait()


def step(features, gain, wq, wk, wv, wo, text):
    images, tokens, width = features.shape
    rows = images * tokens
    hbm = pl.BlockSpec(memory_space=pltpu.HBM)
    vmem = pl.BlockSpec(memory_space=pltpu.VMEM)
    return pl.pallas_call(
        step_kernel,
        out_shape=[
            jax.ShapeDtypeStruct((width, width), BF16),
            jax.ShapeDtypeStruct((images, width), F32),
            jax.ShapeDtypeStruct((1, 128), F32),
        ],
        in_specs=[hbm] * 7,
        out_specs=[vmem, vmem, vmem],
        scratch_shapes=[
            pltpu.VMEM((images, tokens, width), BF16),
            *[pltpu.VMEM((width, width), BF16)] * 4,
            *[pltpu.VMEM((rows, width), BF16)] * 4,
            pltpu.VMEM((images, width), F32),
            pltpu.VMEM((images, width), F32),
            pltpu.VMEM((1, width), F32),
            pltpu.VMEM((images, width), BF16),
            pltpu.SemaphoreType.DMA((images,)),
            pltpu.SemaphoreType.DMA((6,)),
            pltpu.VMEM((32, 8, width), BF16),
            pltpu.VMEM((8, 8, width), BF16),
            pltpu.VMEM((8, 8, width), BF16),
            pltpu.VMEM((32, 8, width), BF16),
            pltpu.VMEM((8, 8, width), BF16),
            pltpu.VMEM((8, 8, 128), F32),
            pltpu.VMEM((32, 1, 256), F32),
            pltpu.VMEM((32, 1, 256), F32),
            pltpu.VMEM((8, 8, 128), F32),
            pltpu.VMEM((8, 64, 128), BF16),
            pltpu.VMEM((8, 64, 128), BF16),
            pltpu.VMEM((8, 8, 128), F32),
            pltpu.VMEM((8, 8, width), BF16),
            pltpu.VMEM((8, 8, width), BF16),
            pltpu.VMEM((32, 32, 128), BF16),
            pltpu.VMEM((32, 32, 128), BF16),
            pltpu.VMEM((32, 1, 128), F32),
            pltpu.SemaphoreType.DMA((16,)),
            pltpu.SemaphoreType.DMA((16,)),
            pltpu.SemaphoreType.DMA((32,)),
            pltpu.SemaphoreType.DMA((16,)),
        ],
        compiler_params=pltpu.CompilerParams(
            collective_id=0, has_side_effects=True, vmem_limit_bytes=40 << 20
        ),
        name="step",
    )(features, gain, wq, wk, wv, wo, text)


def whole(features, ln_gain, w_query, w_key, w_value, w_out, text_raw):
    args = (features, ln_gain.reshape(1, -1), w_query, w_key, w_value, w_out, text_raw)
    wgrad, tgrad, loss = step(*(pltpu.with_memory_space_constraint(v, pltpu.HBM) for v in args))
    return (loss[0, 0], tgrad, wgrad)


def solution(mesh):
    placed = (P("dp", None, None), P(), P(), P(), P(), P(), P("dp", None))
    return jax.shard_map(
        whole, mesh=mesh, in_specs=placed, out_specs=(P(), P("dp", None), P()), check_vma=False
    )
```

```python
import jax
import jax.numpy as jnp
from jax import lax
from jax.experimental import pallas as pl
from jax.experimental.pallas import tpu as pltpu
from jax.sharding import PartitionSpec as P

INV_TEMP = 1.0 / 0.07
EPS = 1e-06
LOG2E = 1.4426950408889634
F32 = jnp.float32
BF16 = jnp.bfloat16
MESH = pl.DeviceIdType.MESH
NT = (((1,), (1,)), ((), ()))
TN = (((0,), (0,)), ((), ()))
NN = (((1,), (0,)), ((), ()))


def dot(a, b, dims=NN):
    return lax.dot_general(a, b, dims, preferred_element_type=F32)


def iota(shape, dim):
    return lax.broadcasted_iota(jnp.int32, shape, dim)


def pack_rows(col):
    lane = iota((8, 128), 1)
    tile = jnp.zeros((8, 128), F32)
    for k in range(8):
        tile = jnp.where(lane == k, col[8 * k : 8 * k + 8], tile)
    return tile


def unpack_rows(tile):
    return jnp.concatenate([tile[:, k : k + 1] for k in range(8)], axis=0)


def rows_of(ref):
    n, eight, width = ref.shape
    return ref[...].astype(F32).reshape(n * eight, width).astype(BF16)


def step_kernel(
    feat_hbm, gain_hbm, wq_hbm, wk_hbm, wv_hbm, wo_hbm, text_hbm,
    wgrad, tgrad_ref, loss_ref,
    feat, wq, wk, wv, wo, normed, qh, kh, vh, abar_f, xbar, gain_v, text_v, fsem, wsem,
    t_all, t_row, u_all, u_col, a_all, rs_all, cs_all, rg_all, cg_all,
    g_send, g_recv, s_all, h_send, h_recv, w_send, w_recv, l_all, send, recv, c1, c2,
):
    div, rem = lax.div, lax.rem
    idx = lax.axis_index("dp")
    core = rem(idx, 2)
    z = rem(div(idx, 2), 8)
    x = rem(div(idx, 16), 4)
    y = div(idx, 64)
    c = x * 2 + core
    r = y * 8 + z
    q = div(idx, 16) * 2 + core

    ys, xs = [[rem(v + i, 4) for i in range(4)] for v in (y, x)]
    zs = [rem(z + j, 8) for j in range(8)]
    other = 1 - core

    def at(y1, x1, z1, core1):
        return (y1 * 64 + x1 * 16 + z1 * 2 + core1,)

    row_group = [
        (xs[i] * 2 + n, at(y, xs[i], z, n))
        for i in (2, 1, 3, 0)
        for n in (other, core)
        if i or n is other
    ]
    far = sorted(
        [(i, j) for i in range(4) for j in range(8) if i or j],
        key=lambda t: -min(t[0], 4 - t[0]) - min(t[1], 8 - t[1]),
    )
    col_group = [(ys[i] * 8 + zs[j], at(ys[i], x, zs[j], core)) for i, j in far]
    ring_group = [(zs[j], at(y, x, zs[j], core)) for j in (4, 3, 5, 2, 6, 1, 7)]
    side_group = [
        (ys[i] * 8 + xs[k] * 2 + n, at(ys[i], xs[k], z, n))
        for i in (2, 1, 3, 0)
        for k in (2, 1, 3, 0)
        for n in (other, core)
        if i or k or n is other
    ]

    a = y * (1 - core) + x * core
    b = x * (1 - core) + y * core

    def place(a1, b1):
        y1 = a1 * (1 - core) + b1 * core
        x1 = b1 * (1 - core) + a1 * core
        return y1, x1

    def device(a1, b1, z1, core1):
        y1, x1 = place(a1, b1)
        return (y1 * 64 + x1 * 16 + z1 * 2 + core1,)

    as_, bs = [[rem(v + i, 4) for i in range(4)] for v in (a, b)]
    partner = (idx + 1 - 2 * core,)

    images = feat.shape[0]
    fcopy = [
        pltpu.make_async_copy(feat_hbm.at[i], feat.at[i], fsem.at[i]) for i in range(images)
    ]
    pairs = ((wq_hbm, wq), (wk_hbm, wk), (wv_hbm, wv), (wo_hbm, wo))
    wcopy = [pltpu.make_async_copy(s, d, wsem.at[i]) for i, (s, d) in enumerate(pairs)]
    gcopy = pltpu.make_async_copy(gain_hbm, gain_v, wsem.at[4])
    tcopy = pltpu.make_async_copy(text_hbm, text_v, wsem.at[5])
    for cp in [gcopy, *fcopy, *wcopy, tcopy]:
        cp.start()

    barrier = pltpu.get_barrier_semaphore()

    def greet(devices):
        for dev in devices:
            pl.semaphore_signal(barrier, inc=1, device_id=dev, device_id_type=MESH)

    greet([dev for _, dev in col_group])
    greet([dev for _, dev in side_group])
    greet([device(as_[i], b, zs[j], core) for i, j in far])

    def push(src, dst, s, dev):
        pltpu.make_async_remote_copy(
            src_ref=src, dst_ref=dst, send_sem=send.at[s], recv_sem=recv.at[s],
            device_id=dev, device_id_type=MESH,
        ).start()

    def share(buf, slot, s, group):
        for _, dev in group:
            push(buf.at[slot], buf.at[slot], s, dev)

    def scatter(src, dst, slot, s, group):
        for p, dev in group:
            push(src.at[p], dst.at[slot], s, dev)

    def local(src, dst, sem):
        return pltpu.make_async_copy(src, dst, sem)

    def arrived(buf, s, n):
        part = buf.at[pl.ds(0, n - 1)]
        local(part, part, recv.at[s]).wait()

    def left(buf, s, n):
        part = buf.at[pl.ds(0, n - 1)]
        local(part, part, send.at[s]).wait()

    gcopy.wait()
    gain = gain_v[...]

    with jax.named_scope("norm"):
        for i in range(images):
            fcopy[i].wait()

            total = jnp.zeros((8, 1024), F32)
            for t in range(2):
                rows = slice(t * 64, t * 64 + 64)
                tok = feat[i, rows, :].astype(F32)
                center = tok - jnp.mean(tok, axis=-1, keepdims=True)
                spread = jnp.mean(center * center, axis=-1, keepdims=True)
                out = center * lax.rsqrt(spread + EPS) * gain
                normed[i * 128 + t * 64 : i * 128 + t * 64 + 64, :] = out.astype(BF16)
                total = total + jnp.sum(tok.reshape(8, 8, 1024), axis=0)
            total = jnp.sum(total, axis=0, keepdims=True)
            first = feat[i, 0:16, :].astype(F32)[0:1]
            xbar[i : i + 1, :] = first + (total - first) * (1.0 / 127.0)

    same_head = jnp.where(
        iota((256, 256), 0) // 64 == iota((256, 256), 1) // 64, 1.0, 0.0
    ).astype(BF16)

    def unit(proj, scale):
        squares = dot((proj * proj).astype(BF16), same_head)
        return (proj * (lax.rsqrt(squares + EPS) * scale)).astype(BF16)

    def project(t, carry):
        cols = pl.ds(pl.multiple_of(t * 256, 256), 256)
        tokens = normed[...]
        query = dot(tokens, wq[:, cols])
        key = dot(tokens, wk[:, cols])
        qh[:, cols] = unit(query, 8.0 * LOG2E)
        kh[:, cols] = unit(key, 1.0)
        vh[:, cols] = dot(tokens, wv[:, cols]).astype(BF16)
        return carry

    with jax.named_scope("project"):
        for i in range(3):
            wcopy[i].wait()
        lax.fori_loop(0, 1, project, 0)

    with jax.named_scope("greet"):
        tcopy.wait()
        text = text_v[...].astype(F32)
        txt_norm = jnp.sqrt(jnp.sum(text * text, axis=1, keepdims=True) + EPS)
        txt_f = text / txt_norm
        txt_u = txt_f.astype(BF16)
        t_all[r] = txt_u
        t_row[z] = txt_u
        pl.semaphore_wait(barrier, 31 + 31 + 31)
        share(t_all, r, 1, col_group)
        share(t_row, z, 12, ring_group)

    with jax.named_scope("project"):
        lax.fori_loop(1, 4, project, 0)

    lane = iota((1, 128), 1)
    low = jnp.where(lane < 64, 1.0, 0.0).astype(BF16)
    high = jnp.where(lane < 64, 0.0, 1.0).astype(BF16)
    weigh = jnp.where(iota((1, 256), 1) % 128 == 0, 1.0, 1.0 / 127.0).astype(F32)
    gather = jnp.where(
        iota((256, 128), 0) // 128 == iota((256, 128), 1) // 64, 1.0, 0.0
    ).astype(BF16)

    def attend(i, carry):
        rows = pl.ds(pl.multiple_of(i * 128, 128), 128)
        pooled = []
        for p in range(8):
            cols = slice(p * 128, p * 128 + 128)
            q = qh[rows, cols]
            both = jnp.concatenate([q * low, q * high], axis=0)
            expo = jnp.exp2(dot(kh[rows, cols], both, NT))
            share_of = expo * (weigh / jnp.sum(expo, axis=0, keepdims=True))
            if p < 4:
                first = jnp.sum(share_of[:, :128], axis=1, keepdims=True)
                second = jnp.sum(share_of[:, 128:], axis=1, keepdims=True)
                pooled.append(jnp.where(lane < 64, first, second))
            else:
                pooled.append(share_of.astype(BF16))
        if pooled[4:]:
            rest = dot(jnp.concatenate(pooled[4:], axis=0), gather)
            pooled[4:] = [rest[p * 128 : p * 128 + 128] for p in range(8 - 4)]
        sums = [
            jnp.sum(
                pooled[p] * vh[rows, p * 128 : p * 128 + 128].astype(F32), axis=0, keepdims=True
            )
            for p in range(8)
        ]
        abar_f[pl.ds(i, 1), :] = jnp.concatenate(sums, axis=1)
        return carry

    with jax.named_scope("attend"):
        lax.fori_loop(0, images, attend, 0)

    with jax.named_scope("emb"):
        abar = abar_f[...].astype(BF16)
        wcopy[3].wait()
        emb = xbar[...] + dot(abar, wo[...])
        emb_norm = jnp.sqrt(jnp.sum(emb * emb, axis=1, keepdims=True) + EPS)
        img_u = (emb / emb_norm).astype(BF16)
        u_all[c] = img_u
        a_all[c] = (abar.astype(F32) / emb_norm).astype(BF16)
        share(u_all, c, 0, row_group)
        share(a_all, c, 2, row_group)
        diag = INV_TEMP * jnp.sum(
            jnp.sum(img_u.astype(F32) * txt_u.astype(F32), axis=1, keepdims=True),
            axis=0, keepdims=True,
        )

    with jax.named_scope("wait_text"):
        arrived(t_all, 1, 32)
    with jax.named_scope("wait_img"):
        arrived(u_all, 0, 8)
    with jax.named_scope("logits"):
        img = rows_of(u_all)
        txt = rows_of(t_all)
        logits = INV_TEMP * dot(img, txt, NT)
        expo = jnp.exp(logits)
        cs_all[r] = jnp.sum(expo, axis=0, keepdims=True)
        share(cs_all, r, 3, col_group)
        rs_all[c] = pack_rows(jnp.sum(expo, axis=1, keepdims=True))
        share(rs_all, c, 4, row_group)
        mine_y = pl.ds(y * 8, 8)
        u_col[mine_y] = u_all[...]
        for i in (2, 1, 3):
            push(u_all, u_col.at[mine_y], 13, at(ys[i], x, z, core))
    with jax.named_scope("wait_sums"):
        arrived(rs_all, 4, 8)
        arrived(cs_all, 3, 32)

    with jax.named_scope("delta"):
        row_tile = jnp.sum(rs_all[...], axis=0)
        colsum = jnp.sum(cs_all[...], axis=0)
        probs = expo * (0.5 / unpack_rows(row_tile) + 0.5 / colsum)
        row = iota((64, 256), 0) - c * 8
        col = iota((64, 256), 1) - r * 8
        same = (row == col) & (row >= 0) & (row < 8)
        delta = (probs - jnp.where(same, 1.0, 0.0)).astype(BF16)
        grad = INV_TEMP * dot(delta, txt)
        for k in range(8):
            g_send[k] = grad[:, 128 * k : 128 * k + 128].astype(BF16)
        g_recv[c] = g_send[c]
        scatter(g_send, g_recv, c, 6, row_group)
        s_part = jnp.sum(delta.astype(F32) * logits, axis=1, keepdims=True)
        my_lane = iota((8, 128), 1) == c
        own_rows = jnp.where(my_lane, row_tile, 0.0)
        own = iota((1, 256), 1) - r * 8
        own_cols = jnp.where((own >= 0) & (own < 8), colsum, 0.0)
        loss = (
            jnp.sum(
                jnp.sum(jnp.log(jnp.where(my_lane, row_tile, 1.0)), axis=1, keepdims=True),
                axis=0, keepdims=True,
            )
            + jnp.sum(
                jnp.log(jnp.where((own >= 0) & (own < 8), colsum, 1.0)), axis=1, keepdims=True
            )
            - 2.0 * diag
        )
        s_all[c] = jnp.where(iota((8, 128), 1) == 8, loss, pack_rows(s_part))
        share(s_all, c, 5, row_group)
        own_row = jnp.sum(own_rows, axis=1, keepdims=True)
        spot = iota((8, 256), 1) - iota((8, 256), 0)
        rg_all[q] = jnp.sum(jnp.where(spot == q * 8, own_row, 0.0), axis=0, keepdims=True)
        share(rg_all, q, 14, side_group)
        own_col = jnp.sum(jnp.where(spot == r * 8, own_cols, 0.0), axis=1, keepdims=True)
        cg_all[z] = jnp.where(iota((8, 128), 1) == z, own_col, 0.0)
        share(cg_all, z, 15, ring_group)

    with jax.named_scope("wait_grad"):
        arrived(s_all, 5, 8)
        arrived(g_recv, 6, 8)
        arrived(a_all, 2, 8)
    with jax.named_scope("wgrad"):
        s_sum = jnp.sum(s_all[...], axis=0)
        my_cols = pl.ds(pl.multiple_of(c * 128, 128), 128)
        f_cols = u_all[:, :, my_cols].astype(F32).reshape(64, 128)
        g_sum = jnp.sum(g_recv[...].astype(F32), axis=0)
        emb_grad = (g_sum - f_cols * unpack_rows(s_sum)).astype(BF16)
        w_send[...] = dot(rows_of(a_all), emb_grad, TN).astype(BF16).reshape(32, 32, 128)
        w_recv[r] = w_send[r]
        scatter(w_send, w_recv, r, 8, col_group)
        l_all[r] = (
            jnp.sum(jnp.where(iota((8, 128), 1) == 8, s_sum, 0.0), axis=0, keepdims=True) * 0.125
        )
        share(l_all, r, 9, col_group)

    with jax.named_scope("wait_bulk"):
        arrived(u_col, 13, 25)
        arrived(t_row, 12, 8)
        arrived(rg_all, 14, 32)
        arrived(cg_all, 15, 8)
    with jax.named_scope("text"):
        every = rows_of(u_col)
        expo_t = jnp.exp(INV_TEMP * dot(rows_of(t_row), every, NT))
        rowsum_t = jnp.sum(rg_all[...], axis=0)
        colsum_t = unpack_rows(jnp.sum(cg_all[...], axis=0))
        probs_t = (expo_t * (0.5 / colsum_t + 0.5 / rowsum_t)).astype(BF16)
        h_send[...] = (INV_TEMP * dot(probs_t, every)).reshape(8, 8, 1024).astype(BF16)
        h_recv[z] = h_send[z]

    with jax.named_scope("wait_w"):
        arrived(w_recv, 8, 32)

    def part(a1, b1, first, size):
        y1, x1 = place(a1, b1)
        return wgrad.at[
            pl.ds(pl.multiple_of(y1 * 256 + first, 32), size),
            pl.ds(pl.multiple_of((x1 * 2 + core) * 128, 128), 128),
        ]

    def block(a1, b1, z1):
        return part(a1, b1, z1 * 32, 32)

    def chunk(a1, b1):
        return part(a1, b1, 0, 256)

    def pass_on(piece, s, arrival, dev):
        pltpu.make_async_remote_copy(
            src_ref=piece, dst_ref=piece, send_sem=send.at[s], recv_sem=arrival,
            device_id=dev, device_id_type=MESH,
        ).start()

    def to_b(piece, a1):
        for m in (2, 1, 3):
            pass_on(piece, 11, c2.at[b * 4 + a1], device(a, bs[m], z, core))

    def to_a(piece, z1):
        for m in (2, 1, 3):
            pass_on(piece, 10, c1.at[a * 8 + z1], device(as_[m], b, z, core))

    near = 4

    def length(t):
        i, j = min(t[0], 4 - t[0]), min(t[1], 8 - t[1])
        return (i + j + (2.5 if i and j > near else 0.0), t)

    order = sorted([(i, j) for i in range(4) for j in range(8) if i or j], key=length)

    with jax.named_scope("first"):
        mine = block(a, b, z)
        mine[...] = jnp.sum(w_recv[...].astype(F32), axis=0).astype(BF16)
        for i, j in order:
            if i == 0 or min(j, 8 - j) <= near:
                pass_on(mine, 10, c1.at[a * 8 + z], device(as_[i], b, zs[j], core))
        to_b(mine, a)

    with jax.named_scope("second"):
        for i, j in order:
            a1, z1 = as_[-i], zs[-j]
            piece = block(a1, b, z1)
            local(piece, piece, c1.at[a1 * 8 + z1]).wait()
            if i == 0 and min(j, 8 - j) > near:
                to_a(piece, z1)
            to_b(piece, a1)
        for k in range(4):
            pass_on(chunk(as_[k], b), 11, recv.at[10], partner)
        scatter(h_send, h_recv, z, 7, ring_group)

    def fourth(t, carry):
        a1, b1 = rem(a + div(t, 3), 4), rem(b + 1 + rem(t, 3), 4)
        piece = chunk(a1, b1)
        local(piece, piece, c2.at[b1 * 4 + a1]).wait()
        pass_on(piece, 11, recv.at[10], partner)
        return carry

    with jax.named_scope("fourth"):
        lax.fori_loop(0, 12, fourth, 0)

    with jax.named_scope("text_out"):
        arrived(h_recv, 7, 8)
        g_txt = jnp.sum(h_recv[...].astype(F32), axis=0) - INV_TEMP * img_u.astype(F32)
        tgrad_ref[...] = (
            g_txt - txt_f * jnp.sum(txt_f * g_txt, axis=1, keepdims=True)
        ) / txt_norm
        arrived(l_all, 9, 32)
        total = jnp.sum(jnp.sum(l_all[...], axis=0), axis=1, keepdims=True)
        loss_ref[...] = jnp.broadcast_to(total * (1.0 / 4096.0), (1, 128))

    with jax.named_scope("drain"):
        half = wgrad.at[pl.ds(0, 512)]
        local(half, half, recv.at[10]).wait()
        left(u_all, 0, 8)
        left(t_all, 1, 32)
        left(a_all, 2, 8)
        left(cs_all, 3, 32)
        left(rs_all, 4, 8)
        left(s_all, 5, 8)
        left(g_send, 6, 8)
        left(h_send, 7, 8)
        left(w_send, 8, 32)
        left(l_all, 9, 32)
        left(t_row, 12, 8)
        left(u_col, 13, 25)
        left(rg_all, 14, 32)
        left(cg_all, 15, 8)
        tall = wgrad.at[pl.ds(0, 992), pl.ds(0, 128)]
        local(tall, tall, send.at[10]).wait()
        wide = wgrad.at[pl.ds(0, 896)]
        local(wide, wide, send.at[11]).wait()


def step(features, gain, wq, wk, wv, wo, text):
    images, tokens, width = features.shape
    rows = images * tokens
    hbm = pl.BlockSpec(memory_space=pltpu.HBM)
    vmem = pl.BlockSpec(memory_space=pltpu.VMEM)
    return pl.pallas_call(
        step_kernel,
        out_shape=[
            jax.ShapeDtypeStruct((width, width), BF16),
            jax.ShapeDtypeStruct((images, width), F32),
            jax.ShapeDtypeStruct((1, 128), F32),
        ],
        in_specs=[hbm] * 7,
        out_specs=[vmem, vmem, vmem],
        scratch_shapes=[
            pltpu.VMEM((images, tokens, width), BF16),
            *[pltpu.VMEM((width, width), BF16)] * 4,
            *[pltpu.VMEM((rows, width), BF16)] * 4,
            pltpu.VMEM((images, width), F32),
            pltpu.VMEM((images, width), F32),
            pltpu.VMEM((1, width), F32),
            pltpu.VMEM((images, width), BF16),
            pltpu.SemaphoreType.DMA((images,)),
            pltpu.SemaphoreType.DMA((6,)),
            pltpu.VMEM((32, 8, width), BF16),
            pltpu.VMEM((8, 8, width), BF16),
            pltpu.VMEM((8, 8, width), BF16),
            pltpu.VMEM((32, 8, width), BF16),
            pltpu.VMEM((8, 8, width), BF16),
            pltpu.VMEM((8, 8, 128), F32),
            pltpu.VMEM((32, 1, 256), F32),
            pltpu.VMEM((32, 1, 256), F32),
            pltpu.VMEM((8, 8, 128), F32),
            pltpu.VMEM((8, 64, 128), BF16),
            pltpu.VMEM((8, 64, 128), BF16),
            pltpu.VMEM((8, 8, 128), F32),
            pltpu.VMEM((8, 8, width), BF16),
            pltpu.VMEM((8, 8, width), BF16),
            pltpu.VMEM((32, 32, 128), BF16),
            pltpu.VMEM((32, 32, 128), BF16),
            pltpu.VMEM((32, 1, 128), F32),
            pltpu.SemaphoreType.DMA((16,)),
            pltpu.SemaphoreType.DMA((16,)),
            pltpu.SemaphoreType.DMA((32,)),
            pltpu.SemaphoreType.DMA((16,)),
        ],
        compiler_params=pltpu.CompilerParams(
            collective_id=0, has_side_effects=True, vmem_limit_bytes=40 << 20
        ),
        name="step",
    )(features, gain, wq, wk, wv, wo, text)


def whole(features, ln_gain, w_query, w_key, w_value, w_out, text_raw):
    args = (features, ln_gain.reshape(1, -1), w_query, w_key, w_value, w_out, text_raw)
    wgrad, tgrad, loss = step(*(pltpu.with_memory_space_constraint(v, pltpu.HBM) for v in args))
    return (loss[0, 0], tgrad, wgrad)


def solution(mesh):
    placed = (P("dp", None, None), P(), P(), P(), P(), P(), P("dp", None))
    return jax.shard_map(
        whole, mesh=mesh, in_specs=placed, out_specs=(P(), P("dp", None), P()), check_vma=False
    )
```

```python
import jax
import jax.numpy as jnp
from jax import lax
from jax.experimental import pallas as pl
from jax.experimental.pallas import tpu as pltpu
from jax.sharding import PartitionSpec as P

INV_TEMP = 1.0 / 0.07
EPS = 1e-06
LOG2E = 1.4426950408889634
F32 = jnp.float32
BF16 = jnp.bfloat16
MESH = pl.DeviceIdType.MESH
NT = (((1,), (1,)), ((), ()))
TN = (((0,), (0,)), ((), ()))
NN = (((1,), (0,)), ((), ()))


def dot(a, b, dims=NN):
    return lax.dot_general(a, b, dims, preferred_element_type=F32)


def iota(shape, dim):
    return lax.broadcasted_iota(jnp.int32, shape, dim)


def pack_rows(col):
    lane = iota((8, 128), 1)
    tile = jnp.zeros((8, 128), F32)
    for k in range(8):
        tile = jnp.where(lane == k, col[8 * k : 8 * k + 8], tile)
    return tile


def unpack_rows(tile):
    return jnp.concatenate([tile[:, k : k + 1] for k in range(8)], axis=0)


def rows_of(ref):
    n, eight, width = ref.shape
    return ref[...].astype(F32).reshape(n * eight, width).astype(BF16)


def step_kernel(
    feat_hbm, gain_hbm, wq_hbm, wk_hbm, wv_hbm, wo_hbm, text_hbm,
    wgrad, tgrad_ref, loss_ref,
    feat, wq, wk, wv, wo, normed, qh, kh, vh, abar_f, xbar, gain_v, text_v, fsem, wsem,
    t_all, t_row, u_all, u_col, a_all, rs_all, cs_all, rg_all, cg_all,
    g_send, g_recv, s_all, h_send, h_recv, w_send, w_recv, l_all, send, recv, c1, c2,
):
    div, rem = lax.div, lax.rem
    idx = lax.axis_index("dp")
    core = rem(idx, 2)
    z = rem(div(idx, 2), 8)
    x = rem(div(idx, 16), 4)
    y = div(idx, 64)
    c = x * 2 + core
    r = y * 8 + z
    q = div(idx, 16) * 2 + core

    ys, xs = [[rem(v + i, 4) for i in range(4)] for v in (y, x)]
    zs = [rem(z + j, 8) for j in range(8)]
    other = 1 - core

    def at(y1, x1, z1, core1):
        return (y1 * 64 + x1 * 16 + z1 * 2 + core1,)

    row_group = [
        (xs[i] * 2 + n, at(y, xs[i], z, n))
        for i in (2, 1, 3, 0)
        for n in (other, core)
        if i or n is other
    ]
    far = sorted(
        [(i, j) for i in range(4) for j in range(8) if i or j],
        key=lambda t: -min(t[0], 4 - t[0]) - min(t[1], 8 - t[1]),
    )
    col_group = [(ys[i] * 8 + zs[j], at(ys[i], x, zs[j], core)) for i, j in far]
    ring_group = [(zs[j], at(y, x, zs[j], core)) for j in (4, 3, 5, 2, 6, 1, 7)]
    side_group = [
        (ys[i] * 8 + xs[k] * 2 + n, at(ys[i], xs[k], z, n))
        for i in (2, 1, 3, 0)
        for k in (2, 1, 3, 0)
        for n in (other, core)
        if i or k or n is other
    ]

    a = y * (1 - core) + x * core
    b = x * (1 - core) + y * core

    def place(a1, b1):
        y1 = a1 * (1 - core) + b1 * core
        x1 = b1 * (1 - core) + a1 * core
        return y1, x1

    def device(a1, b1, z1, core1):
        y1, x1 = place(a1, b1)
        return (y1 * 64 + x1 * 16 + z1 * 2 + core1,)

    as_, bs = [[rem(v + i, 4) for i in range(4)] for v in (a, b)]
    partner = (idx + 1 - 2 * core,)

    images = feat.shape[0]
    fcopy = [
        pltpu.make_async_copy(feat_hbm.at[i], feat.at[i], fsem.at[i]) for i in range(images)
    ]
    pairs = ((wq_hbm, wq), (wk_hbm, wk), (wv_hbm, wv), (wo_hbm, wo))
    wcopy = [pltpu.make_async_copy(s, d, wsem.at[i]) for i, (s, d) in enumerate(pairs)]
    gcopy = pltpu.make_async_copy(gain_hbm, gain_v, wsem.at[4])
    tcopy = pltpu.make_async_copy(text_hbm, text_v, wsem.at[5])
    for cp in [gcopy, *fcopy, *wcopy, tcopy]:
        cp.start()

    barrier = pltpu.get_barrier_semaphore()

    def greet(devices):
        for dev in devices:
            pl.semaphore_signal(barrier, inc=1, device_id=dev, device_id_type=MESH)

    greet([dev for _, dev in col_group])
    greet([dev for _, dev in side_group])
    greet([device(as_[i], b, zs[j], core) for i, j in far])

    def push(src, dst, s, dev):
        pltpu.make_async_remote_copy(
            src_ref=src, dst_ref=dst, send_sem=send.at[s], recv_sem=recv.at[s],
            device_id=dev, device_id_type=MESH,
        ).start()

    def share(buf, slot, s, group):
        for _, dev in group:
            push(buf.at[slot], buf.at[slot], s, dev)

    def scatter(src, dst, slot, s, group):
        for p, dev in group:
            push(src.at[p], dst.at[slot], s, dev)

    def local(src, dst, sem):
        return pltpu.make_async_copy(src, dst, sem)

    def arrived(buf, s, n):
        part = buf.at[pl.ds(0, n - 1)]
        local(part, part, recv.at[s]).wait()

    def left(buf, s, n):
        part = buf.at[pl.ds(0, n - 1)]
        local(part, part, send.at[s]).wait()

    gcopy.wait()
    gain = gain_v[...]

    with jax.named_scope("norm"):
        for i in range(images):
            fcopy[i].wait()

            total = jnp.zeros((8, 1024), F32)
            for t in range(2):
                rows = slice(t * 64, t * 64 + 64)
                tok = feat[i, rows, :].astype(F32)
                center = tok - jnp.mean(tok, axis=-1, keepdims=True)
                spread = jnp.mean(center * center, axis=-1, keepdims=True)
                out = center * lax.rsqrt(spread + EPS) * gain
                normed[i * 128 + t * 64 : i * 128 + t * 64 + 64, :] = out.astype(BF16)
                total = total + jnp.sum(tok.reshape(8, 8, 1024), axis=0)
            total = jnp.sum(total, axis=0, keepdims=True)
            first = feat[i, 0:16, :].astype(F32)[0:1]
            xbar[i : i + 1, :] = first + (total - first) * (1.0 / 127.0)

    same_head = jnp.where(
        iota((256, 256), 0) // 64 == iota((256, 256), 1) // 64, 1.0, 0.0
    ).astype(BF16)

    def unit(proj, scale):
        squares = dot((proj * proj).astype(BF16), same_head)
        return (proj * (lax.rsqrt(squares + EPS) * scale)).astype(BF16)

    def project(t, carry):
        cols = pl.ds(pl.multiple_of(t * 256, 256), 256)
        tokens = normed[...]
        query = dot(tokens, wq[:, cols])
        key = dot(tokens, wk[:, cols])
        qh[:, cols] = unit(query, 8.0 * LOG2E)
        kh[:, cols] = unit(key, 1.0)
        vh[:, cols] = dot(tokens, wv[:, cols]).astype(BF16)
        return carry

    with jax.named_scope("project"):
        for i in range(3):
            wcopy[i].wait()
        lax.fori_loop(0, 1, project, 0)

    with jax.named_scope("greet"):
        tcopy.wait()
        text = text_v[...].astype(F32)
        txt_norm = jnp.sqrt(jnp.sum(text * text, axis=1, keepdims=True) + EPS)
        txt_f = text / txt_norm
        txt_u = txt_f.astype(BF16)
        t_all[r] = txt_u
        t_row[z] = txt_u
        pl.semaphore_wait(barrier, 31 + 31 + 31)
        share(t_all, r, 1, col_group)
        share(t_row, z, 12, ring_group)

    with jax.named_scope("project"):
        lax.fori_loop(1, 4, project, 0)

    lane = iota((1, 128), 1)
    low = jnp.where(lane < 64, 1.0, 0.0).astype(BF16)
    high = jnp.where(lane < 64, 0.0, 1.0).astype(BF16)
    weigh = jnp.where(iota((1, 256), 1) % 128 == 0, 1.0, 1.0 / 127.0).astype(F32)
    gather = jnp.where(
        iota((256, 128), 0) // 128 == iota((256, 128), 1) // 64, 1.0, 0.0
    ).astype(BF16)

    def attend(i, carry):
        rows = pl.ds(pl.multiple_of(i * 128, 128), 128)
        pooled = []
        for p in range(8):
            cols = slice(p * 128, p * 128 + 128)
            q = qh[rows, cols]
            both = jnp.concatenate([q * low, q * high], axis=0)
            expo = jnp.exp2(dot(kh[rows, cols], both, NT))
            share_of = expo * (weigh / jnp.sum(expo, axis=0, keepdims=True))
            if p < 4:
                first = jnp.sum(share_of[:, :128], axis=1, keepdims=True)
                second = jnp.sum(share_of[:, 128:], axis=1, keepdims=True)
                pooled.append(jnp.where(lane < 64, first, second))
            else:
                pooled.append(share_of.astype(BF16))
        if pooled[4:]:
            rest = dot(jnp.concatenate(pooled[4:], axis=0), gather)
            pooled[4:] = [rest[p * 128 : p * 128 + 128] for p in range(8 - 4)]
        sums = [
            jnp.sum(
                pooled[p] * vh[rows, p * 128 : p * 128 + 128].astype(F32), axis=0, keepdims=True
            )
            for p in range(8)
        ]
        abar_f[pl.ds(i, 1), :] = jnp.concatenate(sums, axis=1)
        return carry

    with jax.named_scope("attend"):
        lax.fori_loop(0, images, attend, 0)

    with jax.named_scope("emb"):
        abar = abar_f[...].astype(BF16)
        wcopy[3].wait()
        emb = xbar[...] + dot(abar, wo[...])
        emb_norm = jnp.sqrt(jnp.sum(emb * emb, axis=1, keepdims=True) + EPS)
        img_u = (emb / emb_norm).astype(BF16)
        u_all[c] = img_u
        a_all[c] = (abar.astype(F32) / emb_norm).astype(BF16)
        share(u_all, c, 0, row_group)
        share(a_all, c, 2, row_group)
        diag = INV_TEMP * jnp.sum(
            jnp.sum(img_u.astype(F32) * txt_u.astype(F32), axis=1, keepdims=True),
            axis=0, keepdims=True,
        )

    with jax.named_scope("wait_text"):
        arrived(t_all, 1, 32)
    with jax.named_scope("wait_img"):
        arrived(u_all, 0, 8)
    with jax.named_scope("logits"):
        img = rows_of(u_all)
        txt = rows_of(t_all)
        logits = INV_TEMP * dot(img, txt, NT)
        expo = jnp.exp(logits)
        cs_all[r] = jnp.sum(expo, axis=0, keepdims=True)
        share(cs_all, r, 3, col_group)
        rs_all[c] = pack_rows(jnp.sum(expo, axis=1, keepdims=True))
        share(rs_all, c, 4, row_group)
        mine_y = pl.ds(y * 8, 8)
        u_col[mine_y] = u_all[...]
        for i in (2, 1, 3):
            push(u_all, u_col.at[mine_y], 13, at(ys[i], x, z, core))
    with jax.named_scope("wait_sums"):
        arrived(rs_all, 4, 8)
        arrived(cs_all, 3, 32)

    with jax.named_scope("delta"):
        row_tile = jnp.sum(rs_all[...], axis=0)
        colsum = jnp.sum(cs_all[...], axis=0)
        probs = expo * (0.5 / unpack_rows(row_tile) + 0.5 / colsum)
        row = iota((64, 256), 0) - c * 8
        col = iota((64, 256), 1) - r * 8
        same = (row == col) & (row >= 0) & (row < 8)
        delta = (probs - jnp.where(same, 1.0, 0.0)).astype(BF16)
        grad = INV_TEMP * dot(delta, txt)
        for k in range(8):
            g_send[k] = grad[:, 128 * k : 128 * k + 128].astype(BF16)
        g_recv[c] = g_send[c]
        scatter(g_send, g_recv, c, 6, row_group)
        s_part = jnp.sum(delta.astype(F32) * logits, axis=1, keepdims=True)
        my_lane = iota((8, 128), 1) == c
        own_rows = jnp.where(my_lane, row_tile, 0.0)
        own = iota((1, 256), 1) - r * 8
        own_cols = jnp.where((own >= 0) & (own < 8), colsum, 0.0)
        loss = (
            jnp.sum(
                jnp.sum(jnp.log(jnp.where(my_lane, row_tile, 1.0)), axis=1, keepdims=True),
                axis=0, keepdims=True,
            )
            + jnp.sum(
                jnp.log(jnp.where((own >= 0) & (own < 8), colsum, 1.0)), axis=1, keepdims=True
            )
            - 2.0 * diag
        )
        s_all[c] = jnp.where(iota((8, 128), 1) == 8, loss, pack_rows(s_part))
        share(s_all, c, 5, row_group)
        own_row = jnp.sum(own_rows, axis=1, keepdims=True)
        spot = iota((8, 256), 1) - iota((8, 256), 0)
        rg_all[q] = jnp.sum(jnp.where(spot == q * 8, own_row, 0.0), axis=0, keepdims=True)
        share(rg_all, q, 14, side_group)
        own_col = jnp.sum(jnp.where(spot == r * 8, own_cols, 0.0), axis=1, keepdims=True)
        cg_all[z] = jnp.where(iota((8, 128), 1) == z, own_col, 0.0)
        share(cg_all, z, 15, ring_group)

    with jax.named_scope("wait_grad"):
        arrived(s_all, 5, 8)
        arrived(g_recv, 6, 8)
        arrived(a_all, 2, 8)
    with jax.named_scope("wgrad"):
        s_sum = jnp.sum(s_all[...], axis=0)
        my_cols = pl.ds(pl.multiple_of(c * 128, 128), 128)
        f_cols = u_all[:, :, my_cols].astype(F32).reshape(64, 128)
        g_sum = jnp.sum(g_recv[...].astype(F32), axis=0)
        emb_grad = (g_sum - f_cols * unpack_rows(s_sum)).astype(BF16)
        partial = dot(rows_of(a_all), emb_grad, TN).reshape(32, 2, 16, 128)
        for h in range(2):
            w_send[h] = partial[:, h].astype(BF16)
            w_recv[h, r] = w_send[h, r]
            scatter(w_send.at[h], w_recv.at[h], r, (8, 16)[h], col_group)
        l_all[r] = (
            jnp.sum(jnp.where(iota((8, 128), 1) == 8, s_sum, 0.0), axis=0, keepdims=True) * 0.125
        )
        share(l_all, r, 9, col_group)

    with jax.named_scope("wait_bulk"):
        arrived(u_col, 13, 25)
        arrived(t_row, 12, 8)
        arrived(rg_all, 14, 32)
        arrived(cg_all, 15, 8)
    with jax.named_scope("text"):
        every = rows_of(u_col)
        expo_t = jnp.exp(INV_TEMP * dot(rows_of(t_row), every, NT))
        rowsum_t = jnp.sum(rg_all[...], axis=0)
        colsum_t = unpack_rows(jnp.sum(cg_all[...], axis=0))
        probs_t = (expo_t * (0.5 / colsum_t + 0.5 / rowsum_t)).astype(BF16)
        h_send[...] = (INV_TEMP * dot(probs_t, every)).reshape(8, 8, 1024).astype(BF16)
        h_recv[z] = h_send[z]

    def part(a1, b1, first, size):
        y1, x1 = place(a1, b1)
        return wgrad.at[
            pl.ds(pl.multiple_of(y1 * 256 + first, 16), size),
            pl.ds(pl.multiple_of((x1 * 2 + core) * 128, 128), 128),
        ]

    def block(a1, b1, z1, h):
        return part(a1, b1, z1 * 32 + h * 16, 16)

    def chunk(a1, b1):
        return part(a1, b1, 0, 256)

    def pass_on(piece, s, arrival, dev):
        pltpu.make_async_remote_copy(
            src_ref=piece, dst_ref=piece, send_sem=send.at[s], recv_sem=arrival,
            device_id=dev, device_id_type=MESH,
        ).start()

    def to_b(piece, a1):
        for m in (2, 1, 3):
            pass_on(piece, 11, c2.at[b * 4 + a1], device(a, bs[m], z, core))

    def length(t):
        i, j = min(t[0], 4 - t[0]), min(t[1], 8 - t[1])
        return (i + j, t)

    order = sorted([(i, j) for i in range(4) for j in range(8) if i or j], key=length)

    for h in range(2):
        with jax.named_scope("wait_w"):
            arrived(w_recv.at[h], (8, 16)[h], 32)
        with jax.named_scope("first"):
            mine = block(a, b, z, h)
            mine[...] = jnp.sum(w_recv[h].astype(F32), axis=0).astype(BF16)
            for i, j in order:
                pass_on(mine, 10, c1.at[h, a * 8 + z], device(as_[i], b, zs[j], core))
            to_b(mine, a)

    with jax.named_scope("second"):
        for i, j, h in sorted(
            [(i, j, h) for i, j in order for h in range(2)],
            key=lambda t: (length(t[:2])[0] + 3.0 * t[2], t[2], t),
        ):
            a1, z1 = as_[-i], zs[-j]
            piece = block(a1, b, z1, h)
            local(piece, piece, c1.at[h, a1 * 8 + z1]).wait()
            to_b(piece, a1)
        for k in range(4):
            pass_on(chunk(as_[k], b), 11, recv.at[10], partner)
        scatter(h_send, h_recv, z, 7, ring_group)

    def fourth(t, carry):
        a1, b1 = rem(a + div(t, 3), 4), rem(b + 1 + rem(t, 3), 4)
        piece = chunk(a1, b1)
        local(piece, piece, c2.at[b1 * 4 + a1]).wait()
        pass_on(piece, 11, recv.at[10], partner)
        return carry

    with jax.named_scope("fourth"):
        lax.fori_loop(0, 12, fourth, 0)

    with jax.named_scope("text_out"):
        arrived(h_recv, 7, 8)
        g_txt = jnp.sum(h_recv[...].astype(F32), axis=0) - INV_TEMP * img_u.astype(F32)
        tgrad_ref[...] = (
            g_txt - txt_f * jnp.sum(txt_f * g_txt, axis=1, keepdims=True)
        ) / txt_norm
        arrived(l_all, 9, 32)
        total = jnp.sum(jnp.sum(l_all[...], axis=0), axis=1, keepdims=True)
        loss_ref[...] = jnp.broadcast_to(total * (1.0 / 4096.0), (1, 128))

    with jax.named_scope("drain"):
        half = wgrad.at[pl.ds(0, 512)]
        local(half, half, recv.at[10]).wait()
        left(u_all, 0, 8)
        left(t_all, 1, 32)
        left(a_all, 2, 8)
        left(cs_all, 3, 32)
        left(rs_all, 4, 8)
        left(s_all, 5, 8)
        left(g_send, 6, 8)
        left(h_send, 7, 8)
        left(w_send.at[0], 8, 32)
        left(w_send.at[1], 16, 32)
        left(l_all, 9, 32)
        left(t_row, 12, 8)
        left(u_col, 13, 25)
        left(rg_all, 14, 32)
        left(cg_all, 15, 8)
        tall = wgrad.at[pl.ds(0, 992), pl.ds(0, 128)]
        local(tall, tall, send.at[10]).wait()
        wide = wgrad.at[pl.ds(0, 896)]
        local(wide, wide, send.at[11]).wait()


def step(features, gain, wq, wk, wv, wo, text):
    images, tokens, width = features.shape
    rows = images * tokens
    hbm = pl.BlockSpec(memory_space=pltpu.HBM)
    vmem = pl.BlockSpec(memory_space=pltpu.VMEM)
    return pl.pallas_call(
        step_kernel,
        out_shape=[
            jax.ShapeDtypeStruct((width, width), BF16),
            jax.ShapeDtypeStruct((images, width), F32),
            jax.ShapeDtypeStruct((1, 128), F32),
        ],
        in_specs=[hbm] * 7,
        out_specs=[vmem, vmem, vmem],
        scratch_shapes=[
            pltpu.VMEM((images, tokens, width), BF16),
            *[pltpu.VMEM((width, width), BF16)] * 4,
            *[pltpu.VMEM((rows, width), BF16)] * 4,
            pltpu.VMEM((images, width), F32),
            pltpu.VMEM((images, width), F32),
            pltpu.VMEM((1, width), F32),
            pltpu.VMEM((images, width), BF16),
            pltpu.SemaphoreType.DMA((images,)),
            pltpu.SemaphoreType.DMA((6,)),
            pltpu.VMEM((32, 8, width), BF16),
            pltpu.VMEM((8, 8, width), BF16),
            pltpu.VMEM((8, 8, width), BF16),
            pltpu.VMEM((32, 8, width), BF16),
            pltpu.VMEM((8, 8, width), BF16),
            pltpu.VMEM((8, 8, 128), F32),
            pltpu.VMEM((32, 1, 256), F32),
            pltpu.VMEM((32, 1, 256), F32),
            pltpu.VMEM((8, 8, 128), F32),
            pltpu.VMEM((8, 64, 128), BF16),
            pltpu.VMEM((8, 64, 128), BF16),
            pltpu.VMEM((8, 8, 128), F32),
            pltpu.VMEM((8, 8, width), BF16),
            pltpu.VMEM((8, 8, width), BF16),
            pltpu.VMEM((2, 32, 16, 128), BF16),
            pltpu.VMEM((2, 32, 16, 128), BF16),
            pltpu.VMEM((32, 1, 128), F32),
            pltpu.SemaphoreType.DMA((17,)),
            pltpu.SemaphoreType.DMA((17,)),
            pltpu.SemaphoreType.DMA((2, 32)),
            pltpu.SemaphoreType.DMA((16,)),
        ],
        compiler_params=pltpu.CompilerParams(
            collective_id=0, has_side_effects=True, vmem_limit_bytes=40 << 20
        ),
        name="step",
    )(features, gain, wq, wk, wv, wo, text)


def finish_kernel(w_ref, t_ref, w_out, t_out, sems):
    half = [pl.ds(512 * i, 512) for i in range(2)]
    copies = [pltpu.make_async_copy(w_ref.at[h], w_out.at[h], sems.at[i]) for i, h in enumerate(half)]
    copies.append(pltpu.make_async_copy(t_ref, t_out, sems.at[2]))
    for cp in copies:
        cp.start()
    for cp in copies:
        cp.wait()


def finish(wgrad, tgrad):
    any_spec = pl.BlockSpec(memory_space=pl.ANY)
    hbm = pl.BlockSpec(memory_space=pltpu.HBM)
    return pl.pallas_call(
        finish_kernel,
        out_shape=[jax.ShapeDtypeStruct(v.shape, v.dtype) for v in (wgrad, tgrad)],
        in_specs=[any_spec, any_spec],
        out_specs=[hbm, hbm],
        scratch_shapes=[pltpu.SemaphoreType.DMA((3,))],
        compiler_params=pltpu.CompilerParams(vmem_limit_bytes=1 << 20),
        name="finish",
    )(wgrad, tgrad)


def whole(features, ln_gain, w_query, w_key, w_value, w_out, text_raw):
    args = (features, ln_gain.reshape(1, -1), w_query, w_key, w_value, w_out, text_raw)
    wgrad, tgrad, loss = step(*(pltpu.with_memory_space_constraint(v, pltpu.HBM) for v in args))
    wgrad, tgrad = finish(wgrad, tgrad)
    return (loss[0, 0], tgrad, wgrad)


def solution(mesh):
    placed = (P("dp", None, None), P(), P(), P(), P(), P(), P("dp", None))
    return jax.shard_map(
        whole, mesh=mesh, in_specs=placed, out_specs=(P(), P("dp", None), P()), check_vma=False
    )
```

```python
import jax
import jax.numpy as jnp
from jax import lax
from jax.experimental import pallas as pl
from jax.experimental.pallas import tpu as pltpu
from jax.sharding import PartitionSpec as P

INV_TEMP = 1.0 / 0.07
EPS = 1e-06
LOG2E = 1.4426950408889634
F32 = jnp.float32
BF16 = jnp.bfloat16
MESH = pl.DeviceIdType.MESH
NT = (((1,), (1,)), ((), ()))
TN = (((0,), (0,)), ((), ()))
NN = (((1,), (0,)), ((), ()))


def dot(a, b, dims=NN):
    return lax.dot_general(a, b, dims, preferred_element_type=F32)


def iota(shape, dim):
    return lax.broadcasted_iota(jnp.int32, shape, dim)


def pack_rows(col):
    lane = iota((8, 128), 1)
    tile = jnp.zeros((8, 128), F32)
    for k in range(8):
        tile = jnp.where(lane == k, col[8 * k : 8 * k + 8], tile)
    return tile


def unpack_rows(tile):
    return jnp.concatenate([tile[:, k : k + 1] for k in range(8)], axis=0)


def rows_of(ref):
    n, eight, width = ref.shape
    return ref[...].astype(F32).reshape(n * eight, width).astype(BF16)


def step_kernel(
    feat_hbm, gain_hbm, wq_hbm, wk_hbm, wv_hbm, wo_hbm, text_hbm,
    wgrad, tgrad_ref, loss_ref,
    feat, wq, wk, wv, wo, normed, qh, kh, vh, abar_f, xbar, gain_v, text_v, fsem, wsem,
    txt_v, scaled_t, t_all, t_row, u_all, u_col, a_all, rs_all, cs_all, rg_all, cg_all,
    g_send, g_recv, s_all, h_send, h_recv, w_send, w_recv, l_all, send, recv, c1, c2,
):
    div, rem = lax.div, lax.rem
    idx = lax.axis_index("dp")
    core = rem(idx, 2)
    z = rem(div(idx, 2), 8)
    x = rem(div(idx, 16), 4)
    y = div(idx, 64)
    c = x * 2 + core
    r = y * 8 + z
    q = div(idx, 16) * 2 + core

    ys, xs = [[rem(v + i, 4) for i in range(4)] for v in (y, x)]
    zs = [rem(z + j, 8) for j in range(8)]
    other = 1 - core

    def at(y1, x1, z1, core1):
        return (y1 * 64 + x1 * 16 + z1 * 2 + core1,)

    row_group = [
        (xs[i] * 2 + n, at(y, xs[i], z, n))
        for i in (2, 1, 3, 0)
        for n in (other, core)
        if i or n is other
    ]
    far = sorted(
        [(i, j) for i in range(4) for j in range(8) if i or j],
        key=lambda t: -min(t[0], 4 - t[0]) - min(t[1], 8 - t[1]),
    )
    col_group = [(ys[i] * 8 + zs[j], at(ys[i], x, zs[j], core)) for i, j in far]
    ring_group = [(zs[j], at(y, x, zs[j], core)) for j in (4, 3, 5, 2, 6, 1, 7)]
    side_group = [
        (ys[i] * 8 + xs[k] * 2 + n, at(ys[i], xs[k], z, n))
        for i in (2, 1, 3, 0)
        for k in (2, 1, 3, 0)
        for n in (other, core)
        if i or k or n is other
    ]

    a = y * (1 - core) + x * core
    b = x * (1 - core) + y * core

    def place(a1, b1):
        y1 = a1 * (1 - core) + b1 * core
        x1 = b1 * (1 - core) + a1 * core
        return y1, x1

    def device(a1, b1, z1, core1):
        y1, x1 = place(a1, b1)
        return (y1 * 64 + x1 * 16 + z1 * 2 + core1,)

    as_, bs = [[rem(v + i, 4) for i in range(4)] for v in (a, b)]
    partner = (idx + 1 - 2 * core,)

    images = feat.shape[0]
    fcopy = [
        pltpu.make_async_copy(feat_hbm.at[i], feat.at[i], fsem.at[i]) for i in range(images)
    ]
    pairs = ((wq_hbm, wq), (wk_hbm, wk), (wv_hbm, wv), (wo_hbm, wo))
    wcopy = [pltpu.make_async_copy(s, d, wsem.at[i]) for i, (s, d) in enumerate(pairs)]
    gcopy = pltpu.make_async_copy(gain_hbm, gain_v, wsem.at[4])
    tcopy = pltpu.make_async_copy(text_hbm, text_v, wsem.at[5])
    for cp in [gcopy, *fcopy, *wcopy, tcopy]:
        cp.start()

    barrier = pltpu.get_barrier_semaphore()

    def greet(devices):
        for dev in devices:
            pl.semaphore_signal(barrier, inc=1, device_id=dev, device_id_type=MESH)

    greet([dev for _, dev in col_group])
    greet([dev for _, dev in side_group])
    greet([device(as_[i], b, zs[j], core) for i, j in far])

    def push(src, dst, s, dev):
        pltpu.make_async_remote_copy(
            src_ref=src, dst_ref=dst, send_sem=send.at[s], recv_sem=recv.at[s],
            device_id=dev, device_id_type=MESH,
        ).start()

    def share(buf, slot, s, group):
        for _, dev in group:
            push(buf.at[slot], buf.at[slot], s, dev)

    def scatter(src, dst, slot, s, group):
        for p, dev in group:
            push(src.at[p], dst.at[slot], s, dev)

    def local(src, dst, sem):
        return pltpu.make_async_copy(src, dst, sem)

    def arrived(buf, s, n):
        part = buf.at[pl.ds(0, n - 1)]
        local(part, part, recv.at[s]).wait()

    def left(buf, s, n):
        part = buf.at[pl.ds(0, n - 1)]
        local(part, part, send.at[s]).wait()

    gcopy.wait()
    gain = gain_v[...]

    with jax.named_scope("norm"):
        for i in range(images):
            fcopy[i].wait()

            total = jnp.zeros((8, 1024), F32)
            for t in range(2):
                rows = slice(t * 64, t * 64 + 64)
                tok = feat[i, rows, :].astype(F32)
                center = tok - jnp.mean(tok, axis=-1, keepdims=True)
                spread = jnp.mean(center * center, axis=-1, keepdims=True)
                out = center * lax.rsqrt(spread + EPS) * gain
                normed[i * 128 + t * 64 : i * 128 + t * 64 + 64, :] = out.astype(BF16)
                total = total + jnp.sum(tok.reshape(8, 8, 1024), axis=0)
            total = jnp.sum(total, axis=0, keepdims=True)
            first = feat[i, 0:16, :].astype(F32)[0:1]
            xbar[i : i + 1, :] = first + (total - first) * (1.0 / 127.0)

    same_head = jnp.where(
        iota((256, 256), 0) // 64 == iota((256, 256), 1) // 64, 1.0, 0.0
    ).astype(BF16)

    def unit(proj, scale):
        squares = dot((proj * proj).astype(BF16), same_head)
        return (proj * (lax.rsqrt(squares + EPS) * scale)).astype(BF16)

    def project(t, carry):
        cols = pl.ds(pl.multiple_of(t * 256, 256), 256)
        tokens = normed[...]
        query = dot(tokens, wq[:, cols])
        key = dot(tokens, wk[:, cols])
        qh[:, cols] = unit(query, 8.0 * LOG2E)
        kh[:, cols] = unit(key, 1.0)
        vh[:, cols] = dot(tokens, wv[:, cols]).astype(BF16)
        return carry

    with jax.named_scope("project"):
        for i in range(3):
            wcopy[i].wait()
        lax.fori_loop(0, 1, project, 0)

    with jax.named_scope("greet"):
        tcopy.wait()
        text = text_v[...].astype(F32)
        txt_norm = jnp.sqrt(jnp.sum(text * text, axis=1, keepdims=True) + EPS)
        txt_f = text / txt_norm
        txt_u = txt_f.astype(BF16)
        t_all[r] = txt_u
        t_row[z] = txt_u
        pl.semaphore_wait(barrier, 31 + 31 + 31)
        share(t_all, r, 1, col_group)
        share(t_row, z, 12, ring_group)

    with jax.named_scope("project"):
        lax.fori_loop(1, 4, project, 0)

    lane = iota((1, 128), 1)
    low = jnp.where(lane < 64, 1.0, 0.0).astype(BF16)
    high = jnp.where(lane < 64, 0.0, 1.0).astype(BF16)
    weigh = jnp.where(iota((1, 256), 1) % 128 == 0, 1.0, 1.0 / 127.0).astype(F32)
    gather = jnp.where(
        iota((256, 128), 0) // 128 == iota((256, 128), 1) // 64, 1.0, 0.0
    ).astype(BF16)

    def attend(i, carry):
        rows = pl.ds(pl.multiple_of(i * 128, 128), 128)
        pooled = []
        for p in range(8):
            cols = slice(p * 128, p * 128 + 128)
            q = qh[rows, cols]
            both = jnp.concatenate([q * low, q * high], axis=0)
            expo = jnp.exp2(dot(kh[rows, cols], both, NT))
            share_of = expo * (weigh / jnp.sum(expo, axis=0, keepdims=True))
            if p < 4:
                first = jnp.sum(share_of[:, :128], axis=1, keepdims=True)
                second = jnp.sum(share_of[:, 128:], axis=1, keepdims=True)
                pooled.append(jnp.where(lane < 64, first, second))
            else:
                pooled.append(share_of.astype(BF16))
        if pooled[4:]:
            rest = dot(jnp.concatenate(pooled[4:], axis=0), gather)
            pooled[4:] = [rest[p * 128 : p * 128 + 128] for p in range(8 - 4)]
        sums = [
            jnp.sum(
                pooled[p] * vh[rows, p * 128 : p * 128 + 128].astype(F32), axis=0, keepdims=True
            )
            for p in range(8)
        ]
        abar_f[pl.ds(i, 1), :] = jnp.concatenate(sums, axis=1)
        return carry

    with jax.named_scope("attend"):
        lax.fori_loop(0, images, attend, 0)

    with jax.named_scope("emb"):
        abar = abar_f[...].astype(BF16)
        wcopy[3].wait()
        emb = xbar[...] + dot(abar, wo[...])
        emb_norm = jnp.sqrt(jnp.sum(emb * emb, axis=1, keepdims=True) + EPS)
        img_u = (emb / emb_norm).astype(BF16)
        u_all[c] = img_u
        a_all[c] = (abar.astype(F32) / emb_norm).astype(BF16)
        share(u_all, c, 0, row_group)
        share(a_all, c, 2, row_group)
        diag = INV_TEMP * jnp.sum(
            jnp.sum(img_u.astype(F32) * txt_u.astype(F32), axis=1, keepdims=True),
            axis=0, keepdims=True,
        )

    with jax.named_scope("wait_text"):
        arrived(t_all, 1, 32)
        txt_v[...] = rows_of(t_all)
    with jax.named_scope("wait_img"):
        arrived(u_all, 0, 8)
    with jax.named_scope("logits"):
        img = rows_of(u_all)
        txt = txt_v[...]
        logits = INV_TEMP * dot(img, txt, NT)
        expo = jnp.exp(logits)
        cs_all[r] = jnp.sum(expo, axis=0, keepdims=True)
        share(cs_all, r, 3, col_group)
        rs_all[c] = pack_rows(jnp.sum(expo, axis=1, keepdims=True))
        share(rs_all, c, 4, row_group)
    with jax.named_scope("wait_sums"):
        arrived(rs_all, 4, 8)
        arrived(cs_all, 3, 32)

    with jax.named_scope("delta"):
        row_tile = jnp.sum(rs_all[...], axis=0)
        colsum = jnp.sum(cs_all[...], axis=0)
        probs = expo * (0.5 / unpack_rows(row_tile) + 0.5 / colsum)
        row = iota((64, 256), 0) - c * 8
        col = iota((64, 256), 1) - r * 8
        same = (row == col) & (row >= 0) & (row < 8)
        delta = (probs - jnp.where(same, 1.0, 0.0)).astype(BF16)
        grad = INV_TEMP * dot(delta, txt)
        for k in range(8):
            g_send[k] = grad[:, 128 * k : 128 * k + 128].astype(BF16)
        g_recv[c] = g_send[c]
        scatter(g_send, g_recv, c, 6, row_group)
        s_part = jnp.sum(delta.astype(F32) * logits, axis=1, keepdims=True)
        my_lane = iota((8, 128), 1) == c
        own_rows = jnp.where(my_lane, row_tile, 0.0)
        own = iota((1, 256), 1) - r * 8
        own_cols = jnp.where((own >= 0) & (own < 8), colsum, 0.0)
        loss = (
            jnp.sum(
                jnp.sum(jnp.log(jnp.where(my_lane, row_tile, 1.0)), axis=1, keepdims=True),
                axis=0, keepdims=True,
            )
            + jnp.sum(
                jnp.log(jnp.where((own >= 0) & (own < 8), colsum, 1.0)), axis=1, keepdims=True
            )
            - 2.0 * diag
        )
        s_all[c] = jnp.where(iota((8, 128), 1) == 8, loss, pack_rows(s_part))
        share(s_all, c, 5, row_group)
        own_row = jnp.sum(own_rows, axis=1, keepdims=True)
        spot = iota((8, 256), 1) - iota((8, 256), 0)
        rg_all[q] = jnp.sum(jnp.where(spot == q * 8, own_row, 0.0), axis=0, keepdims=True)
        share(rg_all, q, 14, side_group)
        own_col = jnp.sum(jnp.where(spot == r * 8, own_cols, 0.0), axis=1, keepdims=True)
        cg_all[z] = jnp.where(iota((8, 128), 1) == z, own_col, 0.0)
        share(cg_all, z, 15, ring_group)
        mine_y = pl.ds(y * 8, 8)
        u_col[mine_y] = u_all[...]
        for i in (2, 1, 3):
            push(u_all, u_col.at[mine_y], 13, at(ys[i], x, z, core))

    with jax.named_scope("wait_grad"):
        arrived(a_all, 2, 8)
        scaled_t[...] = rows_of(a_all).T
        arrived(s_all, 5, 8)
        arrived(g_recv, 6, 8)
    with jax.named_scope("wgrad"):
        s_sum = jnp.sum(s_all[...], axis=0)
        my_cols = pl.ds(pl.multiple_of(c * 128, 128), 128)
        f_cols = u_all[:, :, my_cols].astype(F32).reshape(64, 128)
        g_sum = jnp.sum(g_recv[...].astype(F32), axis=0)
        emb_grad = (g_sum - f_cols * unpack_rows(s_sum)).astype(BF16)
        partial = dot(scaled_t[...], emb_grad).reshape(32, 2, 16, 128)
        for h in range(2):
            w_send[h] = partial[:, h].astype(BF16)
            w_recv[h, r] = w_send[h, r]
            scatter(w_send.at[h], w_recv.at[h], r, (8, 16)[h], col_group)
        l_all[r] = (
            jnp.sum(jnp.where(iota((8, 128), 1) == 8, s_sum, 0.0), axis=0, keepdims=True) * 0.125
        )

    def part(a1, b1, first, size):
        y1, x1 = place(a1, b1)
        return wgrad.at[
            pl.ds(pl.multiple_of(y1 * 256 + first, 16), size),
            pl.ds(pl.multiple_of((x1 * 2 + core) * 128, 128), 128),
        ]

    def block(a1, b1, z1, h):
        return part(a1, b1, z1 * 32 + h * 16, 16)

    def chunk(a1, b1):
        return part(a1, b1, 0, 256)

    def pass_on(piece, s, arrival, dev):
        pltpu.make_async_remote_copy(
            src_ref=piece, dst_ref=piece, send_sem=send.at[s], recv_sem=arrival,
            device_id=dev, device_id_type=MESH,
        ).start()

    def to_b(piece, a1):
        for m in (2, 1, 3):
            pass_on(piece, 11, c2.at[b * 4 + a1], device(a, bs[m], z, core))

    def length(t):
        i, j = min(t[0], 4 - t[0]), min(t[1], 8 - t[1])
        return (i + j, t)

    order = sorted([(i, j) for i in range(4) for j in range(8) if i or j], key=length)

    for h in range(2):
        with jax.named_scope("wait_w"):
            arrived(w_recv.at[h], (8, 16)[h], 32)
        with jax.named_scope("first"):
            mine = block(a, b, z, h)
            mine[...] = jnp.sum(w_recv[h].astype(F32), axis=0).astype(BF16)
            for i, j in order:
                pass_on(mine, 10, c1.at[h, a * 8 + z], device(as_[i], b, zs[j], core))
            to_b(mine, a)
        if h == 0:
            with jax.named_scope("wait_bulk"):
                arrived(u_col, 13, 25)
                arrived(t_row, 12, 8)
                arrived(rg_all, 14, 32)
                arrived(cg_all, 15, 8)
            with jax.named_scope("text"):
                every = rows_of(u_col)
                expo_t = jnp.exp(INV_TEMP * dot(rows_of(t_row), every, NT))
                rowsum_t = jnp.sum(rg_all[...], axis=0)
                colsum_t = unpack_rows(jnp.sum(cg_all[...], axis=0))
                probs_t = (expo_t * (0.5 / colsum_t + 0.5 / rowsum_t)).astype(BF16)
                h_send[...] = (INV_TEMP * dot(probs_t, every)).reshape(8, 8, 1024).astype(BF16)
                h_recv[z] = h_send[z]

    with jax.named_scope("second"):
        share(l_all, r, 9, col_group)
        for i, j, h in sorted(
            [(i, j, h) for i, j in order for h in range(2)],
            key=lambda t: (length(t[:2])[0] + 3.0 * t[2], t[2], t),
        ):
            a1, z1 = as_[-i], zs[-j]
            piece = block(a1, b, z1, h)
            local(piece, piece, c1.at[h, a1 * 8 + z1]).wait()
            to_b(piece, a1)
        for k in range(4):
            pass_on(chunk(as_[k], b), 11, recv.at[10], partner)
        scatter(h_send, h_recv, z, 7, ring_group)

    def fourth(t, carry):
        a1, b1 = rem(a + div(t, 3), 4), rem(b + 1 + rem(t, 3), 4)
        piece = chunk(a1, b1)
        local(piece, piece, c2.at[b1 * 4 + a1]).wait()
        pass_on(piece, 11, recv.at[10], partner)
        return carry

    with jax.named_scope("fourth"):
        lax.fori_loop(0, 12, fourth, 0)

    with jax.named_scope("text_out"):
        arrived(h_recv, 7, 8)
        g_txt = jnp.sum(h_recv[...].astype(F32), axis=0) - INV_TEMP * img_u.astype(F32)
        tgrad_ref[...] = (
            g_txt - txt_f * jnp.sum(txt_f * g_txt, axis=1, keepdims=True)
        ) / txt_norm
        arrived(l_all, 9, 32)
        total = jnp.sum(jnp.sum(l_all[...], axis=0), axis=1, keepdims=True)
        loss_ref[...] = jnp.broadcast_to(total * (1.0 / 4096.0), (1, 128))

    with jax.named_scope("drain"):
        half = wgrad.at[pl.ds(0, 512)]
        local(half, half, recv.at[10]).wait()
        left(u_all, 0, 8)
        left(t_all, 1, 32)
        left(a_all, 2, 8)
        left(cs_all, 3, 32)
        left(rs_all, 4, 8)
        left(s_all, 5, 8)
        left(g_send, 6, 8)
        left(h_send, 7, 8)
        left(w_send.at[0], 8, 32)
        left(w_send.at[1], 16, 32)
        left(l_all, 9, 32)
        left(t_row, 12, 8)
        left(u_col, 13, 25)
        left(rg_all, 14, 32)
        left(cg_all, 15, 8)
        tall = wgrad.at[pl.ds(0, 992), pl.ds(0, 128)]
        local(tall, tall, send.at[10]).wait()
        wide = wgrad.at[pl.ds(0, 896)]
        local(wide, wide, send.at[11]).wait()


def step(features, gain, wq, wk, wv, wo, text):
    images, tokens, width = features.shape
    rows = images * tokens
    hbm = pl.BlockSpec(memory_space=pltpu.HBM)
    vmem = pl.BlockSpec(memory_space=pltpu.VMEM)
    return pl.pallas_call(
        step_kernel,
        out_shape=[
            jax.ShapeDtypeStruct((width, width), BF16),
            jax.ShapeDtypeStruct((images, width), F32),
            jax.ShapeDtypeStruct((1, 128), F32),
        ],
        in_specs=[hbm] * 7,
        out_specs=[vmem, vmem, vmem],
        scratch_shapes=[
            pltpu.VMEM((images, tokens, width), BF16),
            *[pltpu.VMEM((width, width), BF16)] * 4,
            *[pltpu.VMEM((rows, width), BF16)] * 4,
            pltpu.VMEM((images, width), F32),
            pltpu.VMEM((images, width), F32),
            pltpu.VMEM((1, width), F32),
            pltpu.VMEM((images, width), BF16),
            pltpu.SemaphoreType.DMA((images,)),
            pltpu.SemaphoreType.DMA((6,)),
            pltpu.VMEM((256, width), BF16),
            pltpu.VMEM((width, 64), BF16),
            pltpu.VMEM((32, 8, width), BF16),
            pltpu.VMEM((8, 8, width), BF16),
            pltpu.VMEM((8, 8, width), BF16),
            pltpu.VMEM((32, 8, width), BF16),
            pltpu.VMEM((8, 8, width), BF16),
            pltpu.VMEM((8, 8, 128), F32),
            pltpu.VMEM((32, 1, 256), F32),
            pltpu.VMEM((32, 1, 256), F32),
            pltpu.VMEM((8, 8, 128), F32),
            pltpu.VMEM((8, 64, 128), BF16),
            pltpu.VMEM((8, 64, 128), BF16),
            pltpu.VMEM((8, 8, 128), F32),
            pltpu.VMEM((8, 8, width), BF16),
            pltpu.VMEM((8, 8, width), BF16),
            pltpu.VMEM((2, 32, 16, 128), BF16),
            pltpu.VMEM((2, 32, 16, 128), BF16),
            pltpu.VMEM((32, 1, 128), F32),
            pltpu.SemaphoreType.DMA((17,)),
            pltpu.SemaphoreType.DMA((17,)),
            pltpu.SemaphoreType.DMA((2, 32)),
            pltpu.SemaphoreType.DMA((16,)),
        ],
        compiler_params=pltpu.CompilerParams(
            collective_id=0, has_side_effects=True, vmem_limit_bytes=40 << 20
        ),
        name="step",
    )(features, gain, wq, wk, wv, wo, text)


def finish_kernel(w_ref, t_ref, w_out, t_out, sems):
    eighth = [pl.ds(128 * i, 128) for i in range(8)]
    copies = [pltpu.make_async_copy(w_ref.at[h], w_out.at[h], sems.at[i]) for i, h in enumerate(eighth)]
    copies.append(pltpu.make_async_copy(t_ref, t_out, sems.at[8]))
    for cp in copies:
        cp.start()
    for cp in copies:
        cp.wait()


def finish(wgrad, tgrad):
    any_spec = pl.BlockSpec(memory_space=pl.ANY)
    hbm = pl.BlockSpec(memory_space=pltpu.HBM)
    return pl.pallas_call(
        finish_kernel,
        out_shape=[jax.ShapeDtypeStruct(v.shape, v.dtype) for v in (wgrad, tgrad)],
        in_specs=[any_spec, any_spec],
        out_specs=[hbm, hbm],
        scratch_shapes=[pltpu.SemaphoreType.DMA((9,))],
        compiler_params=pltpu.CompilerParams(vmem_limit_bytes=1 << 20),
        name="finish",
    )(wgrad, tgrad)


def whole(features, ln_gain, w_query, w_key, w_value, w_out, text_raw):
    args = (features, ln_gain.reshape(1, -1), w_query, w_key, w_value, w_out, text_raw)
    wgrad, tgrad, loss = step(*(pltpu.with_memory_space_constraint(v, pltpu.HBM) for v in args))
    wgrad, tgrad = finish(wgrad, tgrad)
    return (loss[0, 0], tgrad, wgrad)


def solution(mesh):
    placed = (P("dp", None, None), P(), P(), P(), P(), P(), P("dp", None))
    return jax.shard_map(
        whole, mesh=mesh, in_specs=placed, out_specs=(P(), P("dp", None), P()), check_vma=False
    )
```
